8 devices in a mesh: dp: 1 (over z), ep_b: 2 (over y), ep_a: 4 (over x, core).
Axes of the slice: x: 2, y: 2, z: 1, core: 2. Of those that a mesh axis runs over, the one named last changes fastest.
Arguments:
- tokens: bfloat16 [8, 8192, 384], P(('dp', 'ep_b', 'ep_a'))
- expert_ids: int32 [8, 8192], P(('dp', 'ep_b', 'ep_a'))
- route_order: int32 [8, 8192], P(('dp', 'ep_b', 'ep_a'))
- w_route: bfloat16 [384, 256], replicated
- expert_keys: bfloat16 [8, 256], replicated
- temperature: float32 [], replicated
- w_in: bfloat16 [8, 384, 1536], P(('ep_b', 'ep_a'))
- b_in: bfloat16 [8, 1536], P(('ep_b', 'ep_a'))
- w_out: bfloat16 [8, 1536, 384], P(('ep_b', 'ep_a'))
- b_out: bfloat16 [8, 384], P(('ep_b', 'ep_a'))
Outputs:
- output: bfloat16 [8, 8192, 384], P(('dp', 'ep_b', 'ep_a'))
All inputs are finite; a program needn't handle non-finite values.
Results may differ from the reference program's by a relative error of at most 0.002588.
Values are sent between devices in bfloat16 or wider.
A program may use at most 1 GiB of HBM per device.

```python
import jax
import jax.numpy as jnp
from jax import lax

TOKENS_DEV = 8192
MODEL_DIM = 384
HIDDEN_DIM = 1536
ROUTER_DIM = 256
NUM_EXPERTS = 8
CAPACITY = 1280
HOT_SPAN = max(1, NUM_EXPERTS // 4)


def draw_routes(route_key):
    key_list = jax.random.split(route_key, 5)
    shape_ids = (NUM_EXPERTS, TOKENS_DEV)
    spread_ids = jax.random.randint(key_list[0], shape_ids, 0, NUM_EXPERTS)
    hot_pick = jax.random.randint(key_list[1], shape_ids, 0, 4) == 0
    hot_base = jax.random.randint(key_list[2], (NUM_EXPERTS, 1), 0, NUM_EXPERTS)
    hot_ids = (hot_base + jax.random.randint(key_list[3], shape_ids, 0, HOT_SPAN)) % NUM_EXPERTS
    expert_ids = jnp.where(hot_pick, hot_ids, spread_ids).astype(jnp.int32)
    order_keys = jax.random.split(key_list[4], NUM_EXPERTS)
    route_order = jax.vmap(lambda order_key: jax.random.permutation(order_key, TOKENS_DEV))(order_keys)
    return expert_ids, route_order.astype(jnp.int32)


def setup_inputs(seed: int = 0, part: int = 0) -> dict:
    shared_keys = jax.random.split(jax.random.key(seed), 7)
    part_keys = jax.random.split(jax.random.fold_in(jax.random.key(seed + 1), part), 3)
    w_route = jax.random.normal(shared_keys[0], (MODEL_DIM, ROUTER_DIM), jnp.float32) * MODEL_DIM ** -0.5
    expert_keys = jax.random.normal(shared_keys[1], (NUM_EXPERTS, ROUTER_DIM), jnp.float32)
    temperature = jax.random.uniform(shared_keys[2], (), jnp.float32, 0.1, 0.16)
    w_in = jax.random.normal(shared_keys[3], (NUM_EXPERTS, MODEL_DIM, HIDDEN_DIM), jnp.float32) * MODEL_DIM ** -0.5
    b_in = jax.random.normal(shared_keys[4], (NUM_EXPERTS, HIDDEN_DIM), jnp.float32) * 0.5
    w_out = jax.random.normal(shared_keys[5], (NUM_EXPERTS, HIDDEN_DIM, MODEL_DIM), jnp.float32) * HIDDEN_DIM ** -0.5
    b_out = jax.random.normal(shared_keys[6], (NUM_EXPERTS, MODEL_DIM), jnp.float32) * 0.5
    expert_ids, route_order = draw_routes(part_keys[0])
    key_proj = jnp.dot(expert_keys, w_route.T)
    noise_rows = jax.random.normal(part_keys[1], (NUM_EXPERTS, TOKENS_DEV, MODEL_DIM), jnp.float32)
    strength = jax.random.uniform(part_keys[2], (NUM_EXPERTS, TOKENS_DEV, 1), jnp.float32, 0.5, 1.5)
    tokens = noise_rows + strength * key_proj[expert_ids]
    return {
        "tokens": tokens.astype(jnp.bfloat16),
        "expert_ids": expert_ids,
        "route_order": route_order,
        "w_route": w_route.astype(jnp.bfloat16),
        "expert_keys": expert_keys.astype(jnp.bfloat16),
        "temperature": temperature,
        "w_in": w_in.astype(jnp.bfloat16),
        "b_in": b_in.astype(jnp.bfloat16),
        "w_out": w_out.astype(jnp.bfloat16),
        "b_out": b_out.astype(jnp.bfloat16),
    }


def device_route(tok_rows, id_row, order_row, w_route, key_unit, temperature):
    projected = jnp.dot(tok_rows, w_route, preferred_element_type=jnp.float32)
    proj_unit = projected / jnp.sqrt(jnp.sum(projected * projected, axis=1, keepdims=True))
    router_prob = jax.nn.softmax(jnp.dot(proj_unit, key_unit.T) / temperature, axis=1)
    gate_prob = jnp.take_along_axis(router_prob, id_row[:, None], axis=1)[:, 0]
    ranked_ids = id_row[order_row]
    ranked_hot = (ranked_ids[:, None] == jnp.arange(NUM_EXPERTS)[None, :]).astype(jnp.int32)
    ranked_pos = jnp.sum(jnp.cumsum(ranked_hot, axis=0) * ranked_hot, axis=1) - 1
    slot_pos = jnp.zeros((TOKENS_DEV,), jnp.int32).at[order_row].set(ranked_pos)
    dest_slot = jnp.where(slot_pos < CAPACITY, id_row * CAPACITY + slot_pos, NUM_EXPERTS * CAPACITY)
    send_rows = jnp.zeros((NUM_EXPERTS * CAPACITY, MODEL_DIM), jnp.bfloat16).at[dest_slot].set(tok_rows, mode="drop")
    return send_rows, gate_prob, dest_slot


def expert_apply(operands):
    slot_rows, w_first, b_first, w_second, b_second = operands
    hidden = jnp.dot(slot_rows, w_first, preferred_element_type=jnp.float32) + b_first.astype(jnp.float32)
    hidden = jax.nn.gelu(hidden, approximate=False).astype(jnp.bfloat16)
    result = jnp.dot(hidden, w_second, preferred_element_type=jnp.float32) + b_second.astype(jnp.float32)
    return result.astype(jnp.bfloat16)


def reference(tokens, expert_ids, route_order, w_route, expert_keys, temperature, w_in, b_in, w_out, b_out):
    keys_f32 = expert_keys.astype(jnp.float32)
    key_unit = keys_f32 / jnp.sqrt(jnp.sum(keys_f32 * keys_f32, axis=1, keepdims=True))

    def route_one(operands):
        tok_rows, id_row, order_row = operands
        return device_route(tok_rows, id_row, order_row, w_route, key_unit, temperature)

    send_rows, gate_prob, dest_slot = lax.map(route_one, (tokens, expert_ids, route_order))
    grid_rows = send_rows.reshape(NUM_EXPERTS, NUM_EXPERTS, CAPACITY, MODEL_DIM)
    arrived = jnp.swapaxes(grid_rows, 0, 1).reshape(NUM_EXPERTS, NUM_EXPERTS * CAPACITY, MODEL_DIM)
    expert_out = lax.map(expert_apply, (arrived, w_in, b_in, w_out, b_out))
    returned = jnp.swapaxes(expert_out.reshape(NUM_EXPERTS, NUM_EXPERTS, CAPACITY, MODEL_DIM), 0, 1)
    returned = returned.reshape(NUM_EXPERTS, NUM_EXPERTS * CAPACITY, MODEL_DIM)

    def combine_one(operands):
        back_rows, dest_row, gate_row = operands
        picked = jnp.take(back_rows, dest_row, axis=0, mode="fill", fill_value=0)
        return (gate_row[:, None] * picked.astype(jnp.float32)).astype(jnp.bfloat16)

    return lax.map(combine_one, (returned, dest_slot, gate_prob))
```

```python
import functools

import jax
import jax.numpy as jnp
from jax import lax
from jax.experimental import pallas as pl
from jax.experimental.pallas import tpu as pltpu
from jax.sharding import PartitionSpec as P

EXPERT_AXES = ("ep_b", "ep_a")

LANES = 128
BLOCK_ROWS = 4
GRAN = 16
BF16 = jnp.bfloat16
F32 = jnp.float32
NT = (((1,), (1,)), ((), ()))


def iota(shape, dim):
    return lax.broadcasted_iota(jnp.int32, shape, dim)


def plan_kernel(num_experts, capacity, ids_ref, ord_ref, wr_ref, keys_ref, pos_ref, start_ref, count_ref, wt_ref):
    rows = ids_ref.shape[0]
    blocks = rows // BLOCK_ROWS
    place = jnp.zeros((2 * rows, LANES), F32)
    hi_iota = iota((rows, LANES), 0)
    lo_iota = iota((LANES, LANES), 0)
    lane_val = iota((rows, LANES), 1).astype(F32)
    for chunk in range(rows // 8):
        left, right = [], []
        for r in range(8 * chunk, 8 * chunk + 8):
            order_row = ord_ref[r : r + 1, :]
            hit = hi_iota == (order_row >> 7)
            upper = jnp.where(hit, F32(r), 0.0).astype(BF16)
            lower = jnp.where(hit, lane_val, 0.0).astype(BF16)
            left.append(jnp.concatenate([upper, lower], axis=0))
            right.append(jnp.where(lo_iota == (order_row & 127), 1.0, 0.0).astype(BF16))
        place += lax.dot_general(jnp.concatenate(left, axis=1), jnp.concatenate(right, axis=1), NT, preferred_element_type=F32)
    place = (place[:rows] * LANES + place[rows:]).astype(jnp.int32)
    ids = ids_ref[...]
    mask = (ids[None] == iota((num_experts, rows, LANES), 0)).astype(F32)

    def narrow(step, bound):
        trial = bound + (2 * rows * LANES >> (step + 1))
        admitted = jnp.where(place[None] < trial, mask, 0.0)
        total = jnp.sum(jnp.sum(admitted, axis=1, keepdims=True), axis=2, keepdims=True)
        return jnp.where(total <= capacity, trial, bound)

    steps = (rows * LANES).bit_length()
    bound = lax.fori_loop(0, steps, narrow, jnp.zeros((num_experts, 1, 1), jnp.int32))
    kept = jnp.where(place[None] < bound, mask, 0.0)
    kept2 = kept.reshape(num_experts * rows, LANES).astype(BF16)
    before = (iota((LANES, LANES), 0) < iota((LANES, LANES), 1)).astype(BF16)
    lane_prefix = jnp.dot(kept2, before, preferred_element_type=F32)
    row_total = jnp.dot(kept2, jnp.ones((LANES, LANES), BF16), preferred_element_type=F32).astype(BF16)
    row_a, row_b = iota((rows, rows), 0), iota((rows, rows), 1)
    same = row_a // BLOCK_ROWS == row_b // BLOCK_ROWS
    earlier = (same & (row_b < row_a)).astype(BF16)
    same = same.astype(BF16)
    pick = (iota((blocks, rows), 1) == iota((blocks, rows), 0) * BLOCK_ROWS).astype(BF16)
    lane = iota((blocks, LANES), 1)
    slot = jnp.full((rows, LANES), -1, jnp.int32)
    first = jnp.zeros((rows, LANES), jnp.int32)
    starts = jnp.zeros((blocks, LANES), F32)
    counts = jnp.zeros((blocks, LANES), F32)
    for e in range(num_experts):
        part = slice(e * rows, (e + 1) * rows)
        row_prefix = jnp.dot(earlier, row_total[part], preferred_element_type=F32)
        in_block = jnp.dot(same, row_total[part], preferred_element_type=F32).astype(jnp.int32)
        grans = (in_block + (GRAN - 1)) >> 4
        here = first * GRAN + (row_prefix + lane_prefix[part]).astype(jnp.int32)
        slot = jnp.where(kept[e] > 0.0, here, slot)
        starts += jnp.where(lane == e, jnp.dot(pick, first.astype(F32).astype(BF16), preferred_element_type=F32), 0.0)
        counts += jnp.where(lane == e, jnp.dot(pick, grans.astype(F32).astype(BF16), preferred_element_type=F32), 0.0)
        first = first + grans
    pos_ref[...] = slot
    start_ref[...] = starts.astype(jnp.int32)
    count_ref[...] = counts.astype(jnp.int32)
    wr = wr_ref[...]
    router = wr.shape[1]
    eye = (iota((router, router), 0) == iota((router, router), 1)).astype(BF16)
    keys = keys_ref[...].astype(F32)
    unit = keys / jnp.sqrt(jnp.sum(keys * keys, axis=1, keepdims=True))
    folded = lax.dot_general(unit, wr.astype(F32), NT, preferred_element_type=F32, precision=lax.Precision.HIGHEST)
    part_a = folded.astype(BF16)
    rest = folded - part_a.astype(F32)
    part_b = rest.astype(BF16)
    part_c = (rest - part_b.astype(F32)).astype(BF16)
    wt_ref[0:router, :] = lax.dot_general(eye, wr, NT, preferred_element_type=F32).astype(BF16)
    tail = jnp.concatenate([part_a.astype(F32), part_b.astype(F32), part_c.astype(F32), jnp.zeros_like(folded)], axis=0)
    wt_ref[router:, :] = tail.astype(BF16)


def dispatch_kernel(router, num_experts, slots, tau_ref, x_ref, ids_ref, pos_ref, wt_ref, gate_ref, xs_ref):
    rows = ids_ref.shape[0]
    tau = tau_ref[0, 0]
    for sub in range(rows // BLOCK_ROWS):
        row0 = sub * BLOCK_ROWS
        x = x_ref[row0 * LANES : (row0 + BLOCK_ROWS) * LANES, :]
        proj = lax.dot_general(wt_ref[...], x, NT, preferred_element_type=F32)
        square = jnp.sum(proj[:router] * proj[:router], axis=0, keepdims=True)
        ne = num_experts
        logits = proj[router : router + ne] + proj[router + ne : router + 2 * ne] + proj[router + 2 * ne : router + 3 * ne]
        logits = logits / jnp.sqrt(square) / tau
        expo = jnp.exp(logits - jnp.max(logits, axis=0, keepdims=True))
        prob = expo / jnp.sum(expo, axis=0, keepdims=True)
        id_row = jnp.concatenate([ids_ref[r : r + 1, :] for r in range(row0, row0 + BLOCK_ROWS)], axis=1)
        gate = jnp.sum(jnp.where(iota(prob.shape, 0) == id_row, prob, 0.0), axis=0, keepdims=True)
        for r in range(BLOCK_ROWS):
            gate_ref[row0 + r : row0 + r + 1, :] = gate[:, r * LANES : (r + 1) * LANES]
        slot_iota = iota((slots, LANES), 0)
        hot = [(slot_iota == pos_ref[r : r + 1, :]).astype(F32).astype(BF16) for r in range(row0, row0 + BLOCK_ROWS)]
        picked = jnp.dot(jnp.concatenate(hot, axis=1), x, preferred_element_type=F32).astype(BF16)
        grans = slots // GRAN
        xs_ref[sub * grans : (sub + 1) * grans] = picked.reshape(grans, GRAN, picked.shape[1])


def expert_kernel(count, tile, span, eid_ref, start_ref, count_ref, xs_ref, *refs):
    w1_refs, w2_refs = refs[:count], refs[count : 2 * count]
    out_ref = refs[2 * count]
    w1_buf, w2_buf, x_buf, h_buf, table, w_sem, x_sem, y_sem = refs[2 * count + 1 :]
    blocks = start_ref.shape[0]
    width, hidden = w1_buf.shape[1], w1_buf.shape[2]

    def weight_copies(i):
        return (
            pltpu.make_async_copy(w1_refs[i], w1_buf.at[i], w_sem.at[2 * i]),
            pltpu.make_async_copy(w2_refs[i].at[pl.ds(0, w2_buf.shape[1])], w2_buf.at[i], w_sem.at[2 * i + 1]),
        )

    totals = []
    for i in range(count):
        for copy in weight_copies(i):
            copy.start()
        e = eid_ref[0, i]

        def per_block(b, n):
            base = b * span + start_ref[b, e]

            def per_gran(j, n):
                table[i, n] = base + j
                pltpu.make_async_copy(xs_ref.at[base + j], x_buf.at[i, n], x_sem.at[i]).start()
                return n + 1

            return lax.fori_loop(0, count_ref[b, e], per_gran, n)

        totals.append(lax.fori_loop(0, blocks, per_block, 0))
    for i in range(count):
        total = totals[i]
        for copy in weight_copies(i):
            copy.wait()

        def wait_in(j, _):
            pltpu.make_async_copy(xs_ref.at[0], x_buf.at[i, 0], x_sem.at[i]).wait()
            return 0

        lax.fori_loop(0, total, wait_in, 0)
        b1 = jnp.concatenate([w2_buf[i, hidden + r : hidden + r + 1, :] for r in range(hidden // width)], axis=1).astype(F32)
        b2 = w2_buf[i, hidden + hidden // width : hidden + hidden // width + 1, :].astype(F32)

        def per_tile(t, _):
            g0 = t * tile
            x = x_buf[i, pl.ds(g0, tile)].reshape(tile * GRAN, width)
            step = 256
            for c in range(0, hidden, step):
                pre = jnp.dot(x, w1_buf[i, :, c : c + step], preferred_element_type=F32) + b1[:, c : c + step]
                act = 0.5 * pre * (1.0 + lax.erf(pre * F32(0.5**0.5)))
                h_buf[:, c : c + step] = act.astype(BF16)
            y = jnp.dot(h_buf[...], w2_buf[i, 0:hidden, :], preferred_element_type=F32) + b2
            x_buf[i, pl.ds(g0, tile)] = y.astype(BF16).reshape(tile, GRAN, width)

            def out_gran(j, _):
                pltpu.make_async_copy(x_buf.at[i, j], out_ref.at[table[i, j]], y_sem).start()
                return 0

            lax.fori_loop(g0, jnp.minimum(g0 + tile, total), out_gran, 0)
            return 0

        lax.fori_loop(0, (total + tile - 1) // tile, per_tile, 0)

    def wait_out(j, _):
        pltpu.make_async_copy(x_buf.at[0, 0], out_ref.at[0], y_sem).wait()
        return 0

    lax.fori_loop(0, sum(totals), wait_out, 0)


def combine_kernel(slots, ys_ref, pos_ref, gate_ref, out_ref):
    rows = pos_ref.shape[0]
    pos_cols = jnp.transpose(pos_ref[...].astype(F32))
    gate_cols = jnp.transpose(gate_ref[...])
    grans = slots // GRAN
    slot_iota = iota((LANES, slots), 1).astype(F32)
    for sub in range(rows // BLOCK_ROWS):
        row0 = sub * BLOCK_ROWS
        y = ys_ref[sub * grans : (sub + 1) * grans].reshape(slots, ys_ref.shape[2])
        hot = [(slot_iota == pos_cols[:, r : r + 1]).astype(F32).astype(BF16) for r in range(row0, row0 + BLOCK_ROWS)]
        back = jnp.dot(jnp.concatenate(hot, axis=0), y, preferred_element_type=F32)
        for r in range(BLOCK_ROWS):
            at = (row0 + r) * LANES
            scaled = back[r * LANES : (r + 1) * LANES] * gate_cols[:, row0 + r : row0 + r + 1]
            out_ref[at : at + LANES, :] = scaled.astype(BF16)


def vmem():
    return pl.BlockSpec(memory_space=pltpu.VMEM)


def smem():
    return pl.BlockSpec(memory_space=pltpu.SMEM)


def hbm():
    return pl.BlockSpec(memory_space=pl.ANY)


def solution(mesh):
    num_experts = mesh.shape["ep_b"] * mesh.shape["ep_a"]
    tok_spec = P(("dp",) + EXPERT_AXES)
    expert_spec = P(EXPERT_AXES)

    def swap(value, bit):
        return lax.ppermute(value, EXPERT_AXES, [(e, e ^ bit) for e in range(num_experts)])

    def device_step(tokens, expert_ids, route_order, w_route, expert_keys, value_a11, w_in, b_in, w_out, b_out):
        tok_dev, width = tokens.shape[1], tokens.shape[2]
        hidden = w_in.shape[2]
        router = w_route.shape[1]
        capacity = (5 * tok_dev + 4 * num_experts - 1) // (4 * num_experts)
        rows = tok_dev // LANES
        blocks = rows // BLOCK_ROWS
        slots = -(-(BLOCK_ROWS * LANES + num_experts * (GRAN - 1)) // LANES) * LANES
        span = slots // GRAN
        me = lax.axis_index(EXPERT_AXES)

        first = w_in[0]
        bias_rows = jnp.concatenate([b_in[0].reshape(hidden // width, width), b_out, jnp.zeros((7 - hidden // width, width), BF16)], axis=0)
        second = jnp.concatenate([w_out[0], bias_rows], axis=0)
        x_first, y_second = swap(first, 2), swap(second, 4)
        x_second, y_first = swap(second, 2), swap(first, 4)
        d_first, d_second = swap(x_first, 4), swap(y_second, 2)
        groups = []
        for bits, a, b in ((0, first, second), (2, x_first, x_second), (4, y_first, y_second), (6, d_first, d_second)):
            groups.append((bits, (a, swap(a, 1)), (b, swap(b, 1))))

        ids, order = expert_ids.reshape(rows, LANES), route_order.reshape(rows, LANES)
        pos, starts, counts, wt = pl.pallas_call(
            functools.partial(plan_kernel, num_experts, capacity),
            out_shape=(
                jax.ShapeDtypeStruct((rows, LANES), jnp.int32),
                jax.ShapeDtypeStruct((blocks, LANES), jnp.int32),
                jax.ShapeDtypeStruct((blocks, LANES), jnp.int32),
                jax.ShapeDtypeStruct((router + 4 * num_experts, width), BF16),
            ),
            in_specs=[vmem()] * 4,
            out_specs=[vmem()] * 4,
            cost_estimate=pl.CostEstimate(flops=10**9, bytes_accessed=10**6, transcendentals=0),
            name="plan",
        )(ids, order, w_route, expert_keys)

        unit = 2 * BLOCK_ROWS
        gate, xs = pl.pallas_call(
            functools.partial(dispatch_kernel, router, num_experts, slots),
            out_shape=(
                jax.ShapeDtypeStruct((rows, LANES), F32),
                jax.ShapeDtypeStruct((blocks * span, GRAN, width), BF16),
            ),
            grid=(rows // unit,),
            in_specs=[
                smem(),
                pl.BlockSpec((unit * LANES, width), lambda i: (i, 0)),
                pl.BlockSpec((unit, LANES), lambda i: (i, 0)),
                pl.BlockSpec((unit, LANES), lambda i: (i, 0)),
                pl.BlockSpec((router + 4 * num_experts, width), lambda i: (0, 0)),
            ],
            out_specs=(
                pl.BlockSpec((unit, LANES), lambda i: (i, 0)),
                pl.BlockSpec((2 * span, GRAN, width), lambda i: (i, 0, 0)),
            ),
            cost_estimate=pl.CostEstimate(flops=8 * 10**9, bytes_accessed=14 * 10**6, transcendentals=0),
            name="dispatch",
        )(value_a11.reshape(1, 1), tokens[0], ids, pos, wt)

        most = -(-(capacity + blocks * (GRAN - 1)) // (16 * GRAN)) * 16
        tile = 16
        for bits, firsts, seconds in groups:
            eids = jnp.stack([me ^ bits, me ^ bits ^ 1]).reshape(1, 2).astype(jnp.int32)
            n = len(firsts)
            xs = pl.pallas_call(
                functools.partial(expert_kernel, n, tile, span),
                out_shape=jax.ShapeDtypeStruct(xs.shape, BF16),
                in_specs=[smem(), smem(), smem()] + [hbm()] * (1 + 2 * n),
                out_specs=hbm(),
                scratch_shapes=[
                    pltpu.VMEM((n,) + first.shape, BF16),
                    pltpu.VMEM((n,) + second.shape, BF16),
                    pltpu.VMEM((n, most, GRAN, width), BF16),
                    pltpu.VMEM((tile * GRAN, hidden), BF16),
                    pltpu.SMEM((n, most), jnp.int32),
                    pltpu.SemaphoreType.DMA((2 * n,)),
                    pltpu.SemaphoreType.DMA((n,)),
                    pltpu.SemaphoreType.DMA,
                ],
                input_output_aliases={3: 0},
                cost_estimate=pl.CostEstimate(flops=6 * 10**9, bytes_accessed=8 * 10**6, transcendentals=0),
                name=f"experts{bits}",
            )(eids, starts, counts, xs, *firsts, *seconds)

        out = pl.pallas_call(
            functools.partial(combine_kernel, slots),
            out_shape=jax.ShapeDtypeStruct((tok_dev, width), BF16),
            grid=(rows // unit,),
            in_specs=[
                pl.BlockSpec((2 * span, GRAN, width), lambda i: (i, 0, 0)),
                pl.BlockSpec((unit, LANES), lambda i: (i, 0)),
                pl.BlockSpec((unit, LANES), lambda i: (i, 0)),
            ],
            out_specs=pl.BlockSpec((unit * LANES, width), lambda i: (i, 0)),
            cost_estimate=pl.CostEstimate(flops=5 * 10**9, bytes_accessed=14 * 10**6, transcendentals=0),
            name="combine",
        )(xs, pos, gate)
        return out[None]

    return jax.shard_map(
        device_step,
        mesh=mesh,
        in_specs=(tok_spec, tok_spec, tok_spec, P(), P(), P(), expert_spec, expert_spec, expert_spec, expert_spec),
        out_specs=tok_spec,
        check_vma=False,
    )
```

```python
import functools

import jax
import jax.numpy as jnp
from jax import lax
from jax.experimental import pallas as pl
from jax.experimental.pallas import tpu as pltpu
from jax.sharding import PartitionSpec as P

EXPERT_AXES = ("ep_b", "ep_a")

LANES = 128
BLOCK_ROWS = 4
GRAN = 16
BF16 = jnp.bfloat16
F32 = jnp.float32
NT = (((1,), (1,)), ((), ()))


def iota(shape, dim):
    return lax.broadcasted_iota(jnp.int32, shape, dim)


def plan_kernel(num_experts, capacity, ids_ref, ord_ref, wr_ref, keys_ref, pos_ref, start_ref, count_ref, wt_ref):
    rows = ids_ref.shape[0]
    blocks = rows // BLOCK_ROWS
    place = jnp.zeros((2 * rows, LANES), F32)
    hi_iota = iota((rows, LANES), 0)
    lo_iota = iota((LANES, LANES), 0)
    lane_val = iota((rows, LANES), 1).astype(F32)
    for chunk in range(rows // 8):
        left, right = [], []
        for r in range(8 * chunk, 8 * chunk + 8):
            order_row = ord_ref[r : r + 1, :]
            hit = hi_iota == (order_row >> 7)
            upper = jnp.where(hit, F32(r), 0.0).astype(BF16)
            lower = jnp.where(hit, lane_val, 0.0).astype(BF16)
            left.append(jnp.concatenate([upper, lower], axis=0))
            right.append(jnp.where(lo_iota == (order_row & 127), 1.0, 0.0).astype(BF16))
        place += lax.dot_general(jnp.concatenate(left, axis=1), jnp.concatenate(right, axis=1), NT, preferred_element_type=F32)
    place = (place[:rows] * LANES + place[rows:]).astype(jnp.int32)
    ids = ids_ref[...]
    mask = (ids[None] == iota((num_experts, rows, LANES), 0)).astype(F32)

    def narrow(step, bound):
        trial = bound + (2 * rows * LANES >> (step + 1))
        admitted = jnp.where(place[None] < trial, mask, 0.0)
        total = jnp.sum(jnp.sum(admitted, axis=1, keepdims=True), axis=2, keepdims=True)
        return jnp.where(total <= capacity, trial, bound)

    steps = (rows * LANES).bit_length()
    bound = lax.fori_loop(0, steps, narrow, jnp.zeros((num_experts, 1, 1), jnp.int32))
    kept = jnp.where(place[None] < bound, mask, 0.0)
    kept2 = kept.reshape(num_experts * rows, LANES).astype(BF16)
    before = (iota((LANES, LANES), 0) < iota((LANES, LANES), 1)).astype(BF16)
    lane_prefix = jnp.dot(kept2, before, preferred_element_type=F32)
    row_total = jnp.dot(kept2, jnp.ones((LANES, LANES), BF16), preferred_element_type=F32).astype(BF16)
    row_a, row_b = iota((rows, rows), 0), iota((rows, rows), 1)
    same = row_a // BLOCK_ROWS == row_b // BLOCK_ROWS
    earlier = (same & (row_b < row_a)).astype(BF16)
    same = same.astype(BF16)
    pick = (iota((blocks, rows), 1) == iota((blocks, rows), 0) * BLOCK_ROWS).astype(BF16)
    lane = iota((blocks, LANES), 1)
    slot = jnp.full((rows, LANES), -1, jnp.int32)
    first = jnp.zeros((rows, LANES), jnp.int32)
    starts = jnp.zeros((blocks, LANES), F32)
    counts = jnp.zeros((blocks, LANES), F32)
    for e in range(num_experts):
        part = slice(e * rows, (e + 1) * rows)
        row_prefix = jnp.dot(earlier, row_total[part], preferred_element_type=F32)
        in_block = jnp.dot(same, row_total[part], preferred_element_type=F32).astype(jnp.int32)
        grans = (in_block + (GRAN - 1)) >> 4
        here = first * GRAN + (row_prefix + lane_prefix[part]).astype(jnp.int32)
        slot = jnp.where(kept[e] > 0.0, here, slot)
        starts += jnp.where(lane == e, jnp.dot(pick, first.astype(F32).astype(BF16), preferred_element_type=F32), 0.0)
        counts += jnp.where(lane == e, jnp.dot(pick, grans.astype(F32).astype(BF16), preferred_element_type=F32), 0.0)
        first = first + grans
    pos_ref[...] = slot
    start_ref[...] = starts.astype(jnp.int32)
    count_ref[...] = counts.astype(jnp.int32)
    wr = wr_ref[...]
    router = wr.shape[1]
    eye = (iota((router, router), 0) == iota((router, router), 1)).astype(BF16)
    keys = keys_ref[...].astype(F32)
    unit = keys / jnp.sqrt(jnp.sum(keys * keys, axis=1, keepdims=True))
    folded = lax.dot_general(unit, wr.astype(F32), NT, preferred_element_type=F32, precision=lax.Precision.HIGHEST)
    part_a = folded.astype(BF16)
    rest = folded - part_a.astype(F32)
    part_b = rest.astype(BF16)
    part_c = (rest - part_b.astype(F32)).astype(BF16)
    wt_ref[0:router, :] = lax.dot_general(eye, wr, NT, preferred_element_type=F32).astype(BF16)
    tail = jnp.concatenate([part_a.astype(F32), part_b.astype(F32), part_c.astype(F32), jnp.zeros_like(folded)], axis=0)
    wt_ref[router:, :] = tail.astype(BF16)


def dispatch_kernel(router, num_experts, slots, tau_ref, x_ref, ids_ref, pos_ref, wt_ref, gate_ref, xs_ref):
    rows = ids_ref.shape[0]
    tau = tau_ref[0, 0]
    for sub in range(rows // BLOCK_ROWS):
        row0 = sub * BLOCK_ROWS
        x = x_ref[row0 * LANES : (row0 + BLOCK_ROWS) * LANES, :]
        proj = lax.dot_general(wt_ref[...], x, NT, preferred_element_type=F32)
        square = jnp.sum(proj[:router] * proj[:router], axis=0, keepdims=True)
        ne = num_experts
        logits = proj[router : router + ne] + proj[router + ne : router + 2 * ne] + proj[router + 2 * ne : router + 3 * ne]
        logits = logits / jnp.sqrt(square) / tau
        expo = jnp.exp(logits - jnp.max(logits, axis=0, keepdims=True))
        prob = expo / jnp.sum(expo, axis=0, keepdims=True)
        id_row = jnp.concatenate([ids_ref[r : r + 1, :] for r in range(row0, row0 + BLOCK_ROWS)], axis=1)
        gate = jnp.sum(jnp.where(iota(prob.shape, 0) == id_row, prob, 0.0), axis=0, keepdims=True)
        for r in range(BLOCK_ROWS):
            gate_ref[row0 + r : row0 + r + 1, :] = gate[:, r * LANES : (r + 1) * LANES]
        slot_iota = iota((slots, LANES), 0)
        hot = [(slot_iota == pos_ref[r : r + 1, :]).astype(F32).astype(BF16) for r in range(row0, row0 + BLOCK_ROWS)]
        picked = jnp.dot(jnp.concatenate(hot, axis=1), x, preferred_element_type=F32).astype(BF16)
        grans = slots // GRAN
        xs_ref[sub * grans : (sub + 1) * grans] = picked.reshape(grans, GRAN, picked.shape[1])


def load_experts(count, span, eid_ref, start_ref, count_ref, xs_ref, w1_refs, w2_refs, w1_buf, w2_buf, x_buf, w_sem, x_sem):
    totals = []
    for i in range(count):
        pltpu.make_async_copy(w1_refs[i], w1_buf.at[i], w_sem.at[2 * i]).start()
        pltpu.make_async_copy(w2_refs[i], w2_buf.at[i], w_sem.at[2 * i + 1]).start()
        e = eid_ref[0, i]

        def per_block(b, n):
            size = count_ref[b, e]

            @pl.when(size > 0)
            def _():
                run = xs_ref.at[pl.ds(b * span + start_ref[b, e], size)]
                pltpu.make_async_copy(run, x_buf.at[i, pl.ds(n, size)], x_sem.at[i]).start()

            return n + size

        totals.append(lax.fori_loop(0, start_ref.shape[0], per_block, 0))
    return totals


def run_expert(i, total, tile, b1_ref, b2_ref, w1_refs, w2_refs, xs_ref, w1_buf, w2_buf, x_buf, h_buf, w_sem, x_sem):
    width, hidden = w1_buf.shape[1], w1_buf.shape[2]
    pltpu.make_async_copy(w1_refs[i], w1_buf.at[i], w_sem.at[2 * i]).wait()

    @pl.when(total > 0)
    def _():
        pltpu.make_async_copy(xs_ref.at[pl.ds(0, total)], x_buf.at[i, pl.ds(0, total)], x_sem.at[i]).wait()

    pltpu.make_async_copy(w2_refs[i], w2_buf.at[i], w_sem.at[2 * i + 1]).wait()
    b1 = b1_ref[...].astype(F32)
    b2 = b2_ref[...].astype(F32)

    def per_tile(t, _):
        g0 = t * tile
        x = x_buf[i, pl.ds(g0, tile)].reshape(tile * GRAN, width)
        step = 256
        for c in range(0, hidden, step):
            pre = jnp.dot(x, w1_buf[i, :, c : c + step], preferred_element_type=F32) + b1[:, c : c + step]
            act = 0.5 * pre * (1.0 + lax.erf(pre * F32(0.5**0.5)))
            h_buf[:, c : c + step] = act.astype(BF16)
        y = jnp.dot(h_buf[...], w2_buf[i], preferred_element_type=F32) + b2
        x_buf[i, pl.ds(g0, tile)] = y.astype(BF16).reshape(tile, GRAN, width)
        return 0

    lax.fori_loop(0, (total + tile - 1) // tile, per_tile, 0)


def expert_kernel(count, tile, span, eid_ref, start_ref, count_ref, xs_ref, *refs):
    w1_refs, w2_refs = refs[:count], refs[count : 2 * count]
    b1_refs, b2_refs = refs[2 * count : 3 * count], refs[3 * count : 4 * count]
    out_ref = refs[4 * count]
    w1_buf, w2_buf, x_buf, h_buf, w_sem, x_sem, y_sem = refs[4 * count + 1 :]
    totals = load_experts(count, span, eid_ref, start_ref, count_ref, xs_ref, w1_refs, w2_refs, w1_buf, w2_buf, x_buf, w_sem, x_sem)
    for i in range(count):
        run_expert(i, totals[i], tile, b1_refs[i], b2_refs[i], w1_refs, w2_refs, xs_ref, w1_buf, w2_buf, x_buf, h_buf, w_sem, x_sem)
        e = eid_ref[0, i]

        def per_block(b, n):
            size = count_ref[b, e]

            @pl.when(size > 0)
            def _():
                run = out_ref.at[pl.ds(b * span + start_ref[b, e], size)]
                pltpu.make_async_copy(x_buf.at[i, pl.ds(n, size)], run, y_sem.at[i]).start()

            return n + size

        lax.fori_loop(0, start_ref.shape[0], per_block, 0)
    for i in range(count):

        @pl.when(totals[i] > 0)
        def _():
            pltpu.make_async_copy(x_buf.at[i, pl.ds(0, totals[i])], out_ref.at[pl.ds(0, totals[i])], y_sem.at[i]).wait()


def final_kernel(count, tile, span, window, eid_ref, start_ref, count_ref, pos_ref, gate_ref, ids_ref, xs_ref, part_ref, *refs):
    w1_refs, w2_refs = refs[:count], refs[count : 2 * count]
    b1_refs, b2_refs = refs[2 * count : 3 * count], refs[3 * count : 4 * count]
    out_ref = refs[4 * count]
    w1_buf, w2_buf, x_buf, h_buf, o_buf, w_sem, x_sem, p_sem, o_sem = refs[4 * count + 1 :]
    blocks = start_ref.shape[0]
    width = w1_buf.shape[1]
    block_tok = BLOCK_ROWS * LANES
    totals = load_experts(count, span, eid_ref, start_ref, count_ref, xs_ref, w1_refs, w2_refs, w1_buf, w2_buf, x_buf, w_sem, x_sem)
    part_in = pltpu.make_async_copy(part_ref, o_buf, p_sem)
    part_in.start()
    pad = jnp.zeros((tile + window, GRAN, width), BF16)
    for i in range(count):
        x_buf[i, pl.ds(totals[i], tile + window)] = pad
    for i in range(count):
        run_expert(i, totals[i], tile, b1_refs[i], b2_refs[i], w1_refs, w2_refs, xs_ref, w1_buf, w2_buf, x_buf, h_buf, w_sem, x_sem)
    part_in.wait()
    lane = iota((LANES, window * GRAN), 1).astype(F32)

    def out_copy(b):
        rows = pl.ds(pl.multiple_of(b * block_tok, block_tok), block_tok)
        return pltpu.make_async_copy(o_buf.at[rows], out_ref.at[rows], o_sem)

    def per_pair(pair, offsets):
        row0 = pl.multiple_of(pair * 2 * BLOCK_ROWS, 2 * BLOCK_ROWS)
        rows8 = pl.ds(row0, 2 * BLOCK_ROWS)
        pos8, gate8, ids8 = pos_ref[rows8, :], gate_ref[rows8, :], ids_ref[rows8, :]
        gate_cols = jnp.transpose(gate8)
        for sub in range(2):
            b = 2 * pair + sub
            local = []
            longest = 0
            for i in range(count):
                e = eid_ref[0, i]
                mine = jnp.where(ids8 == e, pos8 - start_ref[b, e] * GRAN, -1)
                local.append(jnp.transpose(jnp.where(pos8 < 0, -1, mine).astype(F32)))
                longest = jnp.maximum(longest, count_ref[b, e])

            def per_window(w, _):
                shift = (w * (window * GRAN)).astype(F32)
                ys = jnp.concatenate(
                    [x_buf[i, pl.ds(jnp.minimum(offsets[i] + w * window, totals[i]), window)].reshape(window * GRAN, width) for i in range(count)],
                    axis=0,
                )
                hot = []
                for r in range(sub * BLOCK_ROWS, (sub + 1) * BLOCK_ROWS):
                    hot.append(jnp.concatenate([(lane == local[i][:, r : r + 1] - shift).astype(F32).astype(BF16) for i in range(count)], axis=1))
                back = jnp.dot(jnp.concatenate(hot, axis=0), ys, preferred_element_type=F32)
                for r in range(BLOCK_ROWS):
                    at = pl.ds(pl.multiple_of(b * block_tok + r * LANES, LANES), LANES)
                    scaled = back[r * LANES : (r + 1) * LANES] * gate_cols[:, sub * BLOCK_ROWS + r : sub * BLOCK_ROWS + r + 1]
                    o_buf[at, :] = (o_buf[at, :].astype(F32) + scaled).astype(BF16)
                return 0

            lax.fori_loop(0, (longest + window - 1) // window, per_window, 0)
            out_copy(b).start()
            offsets = tuple(offsets[i] + count_ref[b, eid_ref[0, i]] for i in range(count))
        return offsets

    lax.fori_loop(0, blocks // 2, per_pair, (jnp.int32(0),) * count)
    pltpu.make_async_copy(o_buf, out_ref, o_sem).wait()


def combine_kernel(slots, eid_ref, ys_ref, pos_ref, gate_ref, ids_ref, out_ref):
    rows = pos_ref.shape[0]
    pos_cols = jnp.transpose(pos_ref[...].astype(F32))
    later = (ids_ref[...] == eid_ref[0, 0]) | (ids_ref[...] == eid_ref[0, 1])
    gate_cols = jnp.transpose(jnp.where(later, 0.0, gate_ref[...]))
    grans = slots // GRAN
    slot_iota = iota((LANES, slots), 1).astype(F32)
    for sub in range(rows // BLOCK_ROWS):
        row0 = sub * BLOCK_ROWS
        y = ys_ref[sub * grans : (sub + 1) * grans].reshape(slots, ys_ref.shape[2])
        hot = [(slot_iota == pos_cols[:, r : r + 1]).astype(F32).astype(BF16) for r in range(row0, row0 + BLOCK_ROWS)]
        back = jnp.dot(jnp.concatenate(hot, axis=0), y, preferred_element_type=F32)
        for r in range(BLOCK_ROWS):
            at = (row0 + r) * LANES
            scaled = back[r * LANES : (r + 1) * LANES] * gate_cols[:, row0 + r : row0 + r + 1]
            out_ref[at : at + LANES, :] = scaled.astype(BF16)


def vmem():
    return pl.BlockSpec(memory_space=pltpu.VMEM)


def smem():
    return pl.BlockSpec(memory_space=pltpu.SMEM)


def hbm():
    return pl.BlockSpec(memory_space=pl.ANY)


def solution(mesh):
    num_experts = mesh.shape["ep_b"] * mesh.shape["ep_a"]
    tok_spec = P(("dp",) + EXPERT_AXES)
    expert_spec = P(EXPERT_AXES)

    def swap(value, bit):
        return lax.ppermute(value, EXPERT_AXES, [(e, e ^ bit) for e in range(num_experts)])

    def device_step(tokens, expert_ids, route_order, w_route, expert_keys, value_a11, w_in, b_in, w_out, b_out):
        tok_dev, width = tokens.shape[1], tokens.shape[2]
        hidden = w_in.shape[2]
        router = w_route.shape[1]
        capacity = (5 * tok_dev + 4 * num_experts - 1) // (4 * num_experts)
        rows = tok_dev // LANES
        blocks = rows // BLOCK_ROWS
        slots = -(-(BLOCK_ROWS * LANES + num_experts * (GRAN - 1)) // LANES) * LANES
        span = slots // GRAN
        me = lax.axis_index(EXPERT_AXES)

        first, second = w_in[0], w_out[0]
        x_first, y_second = swap(first, 2), swap(second, 4)
        x_second, y_first = swap(second, 2), swap(first, 4)
        c_first, c_second = swap(first, 1), swap(second, 1)
        bias1 = [b_in] + [swap(b_in, bit) for bit in range(1, num_experts)]
        bias2 = [b_out] + [swap(b_out, bit) for bit in range(1, num_experts)]

        ids, order = expert_ids.reshape(rows, LANES), route_order.reshape(rows, LANES)
        pos, starts, counts, wt = pl.pallas_call(
            functools.partial(plan_kernel, num_experts, capacity),
            out_shape=(
                jax.ShapeDtypeStruct((rows, LANES), jnp.int32),
                jax.ShapeDtypeStruct((blocks, LANES), jnp.int32),
                jax.ShapeDtypeStruct((blocks, LANES), jnp.int32),
                jax.ShapeDtypeStruct((router + 4 * num_experts, width), BF16),
            ),
            in_specs=[vmem()] * 4,
            out_specs=[vmem()] * 4,
            cost_estimate=pl.CostEstimate(flops=10**9, bytes_accessed=10**6, transcendentals=0),
            name="plan",
        )(ids, order, w_route, expert_keys)

        unit = 2 * BLOCK_ROWS
        gate, xs = pl.pallas_call(
            functools.partial(dispatch_kernel, router, num_experts, slots),
            out_shape=(
                jax.ShapeDtypeStruct((rows, LANES), F32),
                jax.ShapeDtypeStruct((blocks * span, GRAN, width), BF16),
            ),
            grid=(rows // unit,),
            in_specs=[
                smem(),
                pl.BlockSpec((unit * LANES, width), lambda i: (i, 0)),
                pl.BlockSpec((unit, LANES), lambda i: (i, 0)),
                pl.BlockSpec((unit, LANES), lambda i: (i, 0)),
                pl.BlockSpec((router + 4 * num_experts, width), lambda i: (0, 0)),
            ],
            out_specs=(
                pl.BlockSpec((unit, LANES), lambda i: (i, 0)),
                pl.BlockSpec((2 * span, GRAN, width), lambda i: (i, 0, 0)),
            ),
            cost_estimate=pl.CostEstimate(flops=8 * 10**9, bytes_accessed=14 * 10**6, transcendentals=0),
            name="dispatch",
        )(value_a11.reshape(1, 1), tokens[0], ids, pos, wt)

        most = -(-(capacity + blocks * (GRAN - 1)) // (16 * GRAN)) * 16
        tile, window = 16, 8

        def eids(bits):
            return jnp.stack([me ^ bits, me ^ bits ^ 1]).reshape(1, 2).astype(jnp.int32)

        def scratch(extra):
            return [
                pltpu.VMEM((2,) + first.shape, BF16),
                pltpu.VMEM((2,) + second.shape, BF16),
                pltpu.VMEM((2, most + extra, GRAN, width), BF16),
                pltpu.VMEM((tile * GRAN, hidden), BF16),
            ]

        def experts(bits, xs, firsts, seconds):
            return pl.pallas_call(
                functools.partial(expert_kernel, 2, tile, span),
                out_shape=jax.ShapeDtypeStruct(xs.shape, BF16),
                in_specs=[smem()] * 3 + [hbm()] * 5 + [vmem()] * 4,
                out_specs=hbm(),
                scratch_shapes=scratch(0)
                + [pltpu.SemaphoreType.DMA((4,)), pltpu.SemaphoreType.DMA((2,)), pltpu.SemaphoreType.DMA((2,))],
                input_output_aliases={3: 0},
                cost_estimate=pl.CostEstimate(flops=6 * 10**9, bytes_accessed=8 * 10**6, transcendentals=0),
                name=f"experts{bits}",
            )(eids(bits), starts, counts, xs, *firsts, *seconds, *bias1[bits : bits + 2], *bias2[bits : bits + 2])

        xs = experts(0, xs, (first, c_first), (second, c_second))
        x_first, y_second, xs = lax.optimization_barrier((x_first, y_second, xs))
        d_first, d_second = swap(x_first, 4), swap(y_second, 2)
        xs = experts(2, xs, (x_first, swap(x_first, 1)), (x_second, swap(x_second, 1)))
        xs = experts(4, xs, (y_first, swap(y_first, 1)), (y_second, swap(y_second, 1)))
        part = pl.pallas_call(
            functools.partial(combine_kernel, slots),
            out_shape=jax.ShapeDtypeStruct((tok_dev, width), BF16),
            grid=(rows // unit,),
            in_specs=[
                smem(),
                pl.BlockSpec((2 * span, GRAN, width), lambda i: (i, 0, 0)),
                pl.BlockSpec((unit, LANES), lambda i: (i, 0)),
                pl.BlockSpec((unit, LANES), lambda i: (i, 0)),
                pl.BlockSpec((unit, LANES), lambda i: (i, 0)),
            ],
            out_specs=pl.BlockSpec((unit * LANES, width), lambda i: (i, 0)),
            cost_estimate=pl.CostEstimate(flops=5 * 10**9, bytes_accessed=14 * 10**6, transcendentals=0),
            name="combine",
        )(eids(6), xs, pos, gate, ids)
        d_first, d_second, part = lax.optimization_barrier((d_first, d_second, part))
        out = pl.pallas_call(
            functools.partial(final_kernel, 2, tile, span, window),
            out_shape=jax.ShapeDtypeStruct((tok_dev, width), BF16),
            in_specs=[smem()] * 3 + [vmem()] * 3 + [hbm()] * 6 + [vmem()] * 4,
            out_specs=hbm(),
            scratch_shapes=scratch(tile + window)
            + [
                pltpu.VMEM((tok_dev, width), BF16),
                pltpu.SemaphoreType.DMA((4,)),
                pltpu.SemaphoreType.DMA((2,)),
                pltpu.SemaphoreType.DMA,
                pltpu.SemaphoreType.DMA,
            ],
            cost_estimate=pl.CostEstimate(flops=7 * 10**9, bytes_accessed=8 * 10**6, transcendentals=0),
            name="final",
        )(
            eids(6), starts, counts, pos, gate, ids, xs, part, d_first, swap(d_first, 1), d_second, swap(d_second, 1),
            *bias1[6:8], *bias2[6:8],
        )
        return out[None]

    return jax.shard_map(
        device_step,
        mesh=mesh,
        in_specs=(tok_spec, tok_spec, tok_spec, P(), P(), P(), expert_spec, expert_spec, expert_spec, expert_spec),
        out_specs=tok_spec,
        check_vma=False,
    )
```

```python
import functools

import jax
import jax.numpy as jnp
from jax import lax
from jax.experimental import pallas as pl
from jax.experimental.pallas import tpu as pltpu
from jax.sharding import PartitionSpec as P


EXPERT_AXES = ("ep_b", "ep_a")

LANES = 128
BLOCK_ROWS = 4
GRAN = 16
BF16 = jnp.bfloat16
F32 = jnp.float32
NT = (((1,), (1,)), ((), ()))


def iota(shape, dim):
    return lax.broadcasted_iota(jnp.int32, shape, dim)


def plan_step(num_experts, capacity, ids_ref, ord_ref, wr_ref, keys_ref, pos_ref, start_ref, count_ref, wt_ref):
    rows = ids_ref.shape[0]
    blocks = rows // BLOCK_ROWS
    place = jnp.zeros((2 * rows, LANES), F32)
    hi_iota = iota((rows, LANES), 0)
    lo_iota = iota((LANES, LANES), 0)
    lane_val = iota((rows, LANES), 1).astype(F32)
    for chunk in range(rows // 8):
        left, right = [], []
        for r in range(8 * chunk, 8 * chunk + 8):
            order_row = ord_ref[r : r + 1, :]
            hit = hi_iota == (order_row >> 7)
            upper = jnp.where(hit, F32(r), 0.0).astype(BF16)
            lower = jnp.where(hit, lane_val, 0.0).astype(BF16)
            left.append(jnp.concatenate([upper, lower], axis=0))
            right.append(jnp.where(lo_iota == (order_row & 127), 1.0, 0.0).astype(BF16))
        place += lax.dot_general(jnp.concatenate(left, axis=1), jnp.concatenate(right, axis=1), NT, preferred_element_type=F32)
    place = (place[:rows] * LANES + place[rows:]).astype(jnp.int32)
    ids = ids_ref[...]
    mask = (ids[None] == iota((num_experts, rows, LANES), 0)).astype(F32)

    def narrow(step, bound):
        trial = bound + (2 * rows * LANES >> (step + 1))
        admitted = jnp.where(place[None] < trial, mask, 0.0)
        total = jnp.sum(jnp.sum(admitted, axis=1, keepdims=True), axis=2, keepdims=True)
        return jnp.where(total <= capacity, trial, bound)

    steps = (rows * LANES).bit_length()
    bound = lax.fori_loop(0, steps, narrow, jnp.zeros((num_experts, 1, 1), jnp.int32))
    kept = jnp.where(place[None] < bound, mask, 0.0)
    kept2 = kept.reshape(num_experts * rows, LANES).astype(BF16)
    before = (iota((LANES, LANES), 0) < iota((LANES, LANES), 1)).astype(BF16)
    lane_prefix = jnp.dot(kept2, before, preferred_element_type=F32)
    row_total = jnp.dot(kept2, jnp.ones((LANES, LANES), BF16), preferred_element_type=F32).astype(BF16)
    row_a, row_b = iota((rows, rows), 0), iota((rows, rows), 1)
    same = row_a // BLOCK_ROWS == row_b // BLOCK_ROWS
    earlier = (same & (row_b < row_a)).astype(BF16)
    same = same.astype(BF16)
    pick = (iota((blocks, rows), 1) == iota((blocks, rows), 0) * BLOCK_ROWS).astype(BF16)
    lane = iota((blocks, LANES), 1)
    slot = jnp.full((rows, LANES), -1, jnp.int32)
    first = jnp.zeros((rows, LANES), jnp.int32)
    starts = jnp.zeros((blocks, LANES), F32)
    counts = jnp.zeros((blocks, LANES), F32)
    for e in range(num_experts):
        part = slice(e * rows, (e + 1) * rows)
        row_prefix = jnp.dot(earlier, row_total[part], preferred_element_type=F32)
        in_block = jnp.dot(same, row_total[part], preferred_element_type=F32).astype(jnp.int32)
        grans = (in_block + (GRAN - 1)) >> 4
        here = first * GRAN + (row_prefix + lane_prefix[part]).astype(jnp.int32)
        slot = jnp.where(kept[e] > 0.0, here, slot)
        starts += jnp.where(lane == e, jnp.dot(pick, first.astype(F32).astype(BF16), preferred_element_type=F32), 0.0)
        counts += jnp.where(lane == e, jnp.dot(pick, grans.astype(F32).astype(BF16), preferred_element_type=F32), 0.0)
        first = first + grans
    pos_ref[...] = slot
    start_ref[...] = starts.astype(jnp.int32)
    count_ref[...] = counts.astype(jnp.int32)
    wr = wr_ref[...]
    router = wr.shape[1]
    eye = (iota((router, router), 0) == iota((router, router), 1)).astype(BF16)
    keys = keys_ref[...].astype(F32)
    unit = keys / jnp.sqrt(jnp.sum(keys * keys, axis=1, keepdims=True))
    folded = lax.dot_general(unit, wr.astype(F32), NT, preferred_element_type=F32, precision=lax.Precision.HIGHEST)
    part_a = folded.astype(BF16)
    rest = folded - part_a.astype(F32)
    part_b = rest.astype(BF16)
    part_c = (rest - part_b.astype(F32)).astype(BF16)
    wt_ref[0:router, :] = lax.dot_general(eye, wr, NT, preferred_element_type=F32).astype(BF16)
    tail = jnp.concatenate([part_a.astype(F32), part_b.astype(F32), part_c.astype(F32), jnp.zeros_like(folded)], axis=0)
    wt_ref[router:, :] = tail.astype(BF16)


def dispatch_kernel(
    router, num_experts, capacity, slots, tau_ref, ids_ref, ord_ref, wr_ref, keys_ref, x_ref,
    pos_ref, start_ref, count_ref, gate_ref, xs_ref, wt_ref,
):
    @pl.when(pl.program_id(0) == 0)
    def _():
        plan_step(num_experts, capacity, ids_ref, ord_ref, wr_ref, keys_ref, pos_ref, start_ref, count_ref, wt_ref)

    rows = x_ref.shape[0] // LANES
    part = pl.ds(pl.multiple_of(pl.program_id(0) * rows, rows), rows)
    ids, pos = ids_ref[part, :], pos_ref[part, :]
    tau = tau_ref[0, 0]
    for sub in range(rows // BLOCK_ROWS):
        row0 = sub * BLOCK_ROWS
        x = x_ref[row0 * LANES : (row0 + BLOCK_ROWS) * LANES, :]
        proj = lax.dot_general(wt_ref[...], x, NT, preferred_element_type=F32)
        square = jnp.sum(proj[:router] * proj[:router], axis=0, keepdims=True)
        ne = num_experts
        logits = proj[router : router + ne] + proj[router + ne : router + 2 * ne] + proj[router + 2 * ne : router + 3 * ne]
        logits = logits / jnp.sqrt(square) / tau
        expo = jnp.exp(logits - jnp.max(logits, axis=0, keepdims=True))
        prob = expo / jnp.sum(expo, axis=0, keepdims=True)
        id_row = jnp.concatenate([ids[r : r + 1] for r in range(row0, row0 + BLOCK_ROWS)], axis=1)
        gate = jnp.sum(jnp.where(iota(prob.shape, 0) == id_row, prob, 0.0), axis=0, keepdims=True)
        for r in range(BLOCK_ROWS):
            gate_ref[row0 + r : row0 + r + 1, :] = gate[:, r * LANES : (r + 1) * LANES]
        slot_iota = iota((slots, LANES), 0)
        hot = [(slot_iota == pos[r : r + 1]).astype(F32).astype(BF16) for r in range(row0, row0 + BLOCK_ROWS)]
        picked = jnp.dot(jnp.concatenate(hot, axis=1), x, preferred_element_type=F32).astype(BF16)
        grans = slots // GRAN
        xs_ref[sub * grans : (sub + 1) * grans] = picked.reshape(grans, GRAN, picked.shape[1])


def load_expert(i, span, eid_ref, start_ref, count_ref, xs_ref, w1_refs, w2_refs, w1_buf, w2_buf, x_buf, w_sem, x_sem):
    pltpu.make_async_copy(w1_refs[i], w1_buf.at[i], w_sem.at[2 * i]).start()
    e = eid_ref[0, i]

    def per_block(b, n):
        size = count_ref[b, e]

        @pl.when(size > 0)
        def _():
            run = xs_ref.at[pl.ds(b * span + start_ref[b, e], size)]
            pltpu.make_async_copy(run, x_buf.at[i, pl.ds(n, size)], x_sem.at[i]).start()

        return n + size

    total = lax.fori_loop(0, start_ref.shape[0], per_block, 0)
    pltpu.make_async_copy(w2_refs[i], w2_buf.at[i], w_sem.at[2 * i + 1]).start()
    return total


def run_expert(i, total, tile, b_ref, w1_refs, w2_refs, xs_ref, w1_buf, w2_buf, x_buf, h_buf, w_sem, x_sem):
    width, hidden = w1_buf.shape[1], w1_buf.shape[2]
    pltpu.make_async_copy(w1_refs[i], w1_buf.at[i], w_sem.at[2 * i]).wait()

    @pl.when(total > 0)
    def _():
        pltpu.make_async_copy(xs_ref.at[pl.ds(0, total)], x_buf.at[i, pl.ds(0, total)], x_sem.at[i]).wait()

    pltpu.make_async_copy(w2_refs[i], w2_buf.at[i], w_sem.at[2 * i + 1]).wait()
    b1 = b_ref[:, 0:hidden].astype(F32)
    b2 = b_ref[:, hidden : hidden + width].astype(F32)

    def per_tile(t, _):
        g0 = t * tile
        x = x_buf[i, pl.ds(g0, tile)].reshape(tile * GRAN, width)
        step = 256
        for c in range(0, hidden, step):
            pre = jnp.dot(x, w1_buf[i, :, c : c + step], preferred_element_type=F32) + b1[:, c : c + step]
            act = 0.5 * pre * (1.0 + lax.erf(pre * F32(0.5**0.5)))
            h_buf[:, c : c + step] = act.astype(BF16)
        y = jnp.dot(h_buf[...], w2_buf[i], preferred_element_type=F32) + b2
        x_buf[i, pl.ds(g0, tile)] = y.astype(BF16).reshape(tile, GRAN, width)
        return 0

    lax.fori_loop(0, (total + tile - 1) // tile, per_tile, 0)


def expert_kernel(count, tile, span, eid_ref, start_ref, count_ref, xs_ref, *refs):
    w1_refs, w2_refs, b_refs = refs[:count], refs[count : 2 * count], refs[2 * count : 3 * count]
    out_ref = refs[3 * count]
    w1_buf, w2_buf, x_buf, h_buf, w_sem, x_sem, y_sem = refs[3 * count + 1 :]

    def load(i):
        return load_expert(i, span, eid_ref, start_ref, count_ref, xs_ref, w1_refs, w2_refs, w1_buf, w2_buf, x_buf, w_sem, x_sem)

    totals = [load(0)]
    for i in range(count):
        if i + 1 < count:
            totals.append(load(i + 1))
        run_expert(i, totals[i], tile, b_refs[i], w1_refs, w2_refs, xs_ref, w1_buf, w2_buf, x_buf, h_buf, w_sem, x_sem)
        e = eid_ref[0, i]

        def per_block(b, n):
            size = count_ref[b, e]

            @pl.when(size > 0)
            def _():
                run = out_ref.at[pl.ds(b * span + start_ref[b, e], size)]
                pltpu.make_async_copy(x_buf.at[i, pl.ds(n, size)], run, y_sem.at[i]).start()

            return n + size

        lax.fori_loop(0, start_ref.shape[0], per_block, 0)
    for i in range(count):

        @pl.when(totals[i] > 0)
        def _():
            pltpu.make_async_copy(x_buf.at[i, pl.ds(0, totals[i])], out_ref.at[pl.ds(0, totals[i])], y_sem.at[i]).wait()


def final_kernel(count, tile, span, window, eid_ref, start_ref, count_ref, pos_ref, gate_ref, ids_ref, xs_ref, part_ref, *refs):
    w1_refs, w2_refs, b_refs = refs[:count], refs[count : 2 * count], refs[2 * count : 3 * count]
    out_ref = refs[3 * count]
    w1_buf, w2_buf, x_buf, h_buf, w_sem, x_sem, o_buf, p_sem, o_sem = refs[3 * count + 1 :]
    blocks = start_ref.shape[0]
    width = w1_buf.shape[1]
    block_tok = BLOCK_ROWS * LANES

    def load(i):
        return load_expert(i, span, eid_ref, start_ref, count_ref, xs_ref, w1_refs, w2_refs, w1_buf, w2_buf, x_buf, w_sem, x_sem)

    totals = [load(i) for i in range(count)]
    part_in = pltpu.make_async_copy(part_ref, o_buf, p_sem)
    part_in.start()
    pad = jnp.zeros((tile + window, GRAN, width), BF16)
    for i in range(count):
        x_buf[i, pl.ds(totals[i], tile + window)] = pad
    for i in range(count):
        run_expert(i, totals[i], tile, b_refs[i], w1_refs, w2_refs, xs_ref, w1_buf, w2_buf, x_buf, h_buf, w_sem, x_sem)
    part_in.wait()
    lane = iota((LANES, window * GRAN), 1).astype(F32)

    def out_copy(b):
        rows = pl.ds(pl.multiple_of(b * block_tok, block_tok), block_tok)
        return pltpu.make_async_copy(o_buf.at[rows], out_ref.at[rows], o_sem)

    def per_pair(pair, offsets):
        row0 = pl.multiple_of(pair * 2 * BLOCK_ROWS, 2 * BLOCK_ROWS)
        rows8 = pl.ds(row0, 2 * BLOCK_ROWS)
        pos8, gate8, ids8 = pos_ref[rows8, :], gate_ref[rows8, :], ids_ref[rows8, :]
        gate_cols = jnp.transpose(gate8)
        upper = iota(pos8.shape, 0) < BLOCK_ROWS
        local = []
        for i in range(count):
            e = eid_ref[0, i]
            origin = jnp.where(upper, start_ref[2 * pair, e], start_ref[2 * pair + 1, e]) * GRAN
            mine = (ids8 == e) & (pos8 >= 0)
            local.append(jnp.transpose(jnp.where(mine, pos8 - origin, -1).astype(F32)))

        def window_rows(sub, w, offsets):
            ys = jnp.concatenate(
                [x_buf[i, pl.ds(jnp.minimum(offsets[i] + w * window, totals[i]), window)].reshape(window * GRAN, width) for i in range(count)],
                axis=0,
            )
            shift = jnp.asarray(w * (window * GRAN)).astype(F32)
            hot = []
            for r in range(sub * BLOCK_ROWS, (sub + 1) * BLOCK_ROWS):
                hot.append(jnp.concatenate([(lane == local[i][:, r : r + 1] - shift).astype(F32).astype(BF16) for i in range(count)], axis=1))
            return jnp.dot(jnp.concatenate(hot, axis=0), ys, preferred_element_type=F32)

        def add(sub, back):
            for r in range(BLOCK_ROWS):
                at = pl.ds(pl.multiple_of((2 * pair + sub) * block_tok + r * LANES, LANES), LANES)
                scaled = back[r * LANES : (r + 1) * LANES] * gate_cols[:, sub * BLOCK_ROWS + r : sub * BLOCK_ROWS + r + 1]
                o_buf[at, :] = (o_buf[at, :].astype(F32) + scaled).astype(BF16)

        starts = [offsets]
        for sub in range(2):
            starts.append(tuple(starts[sub][i] + count_ref[2 * pair + sub, eid_ref[0, i]] for i in range(count)))
        for sub in range(2):
            add(sub, window_rows(sub, 0, starts[sub]))
        for sub in range(2):
            longest = starts[sub + 1][0] - starts[sub][0]
            for i in range(1, count):
                longest = jnp.maximum(longest, starts[sub + 1][i] - starts[sub][i])

            def more(w, _):
                add(sub, window_rows(sub, w, starts[sub]))
                return 0

            lax.fori_loop(1, (longest + window - 1) // window, more, 0)
            out_copy(2 * pair + sub).start()
        return starts[2]

    lax.fori_loop(0, blocks // 2, per_pair, (jnp.int32(0),) * count)
    pltpu.make_async_copy(o_buf, out_ref, o_sem).wait()


def combine_kernel(slots, eid_ref, ys_ref, pos_ref, gate_ref, ids_ref, out_ref):
    rows = pos_ref.shape[0]
    pos_cols = jnp.transpose(pos_ref[...].astype(F32))
    later = (ids_ref[...] == eid_ref[0, 0]) | (ids_ref[...] == eid_ref[0, 1])
    gate_cols = jnp.transpose(jnp.where(later, 0.0, gate_ref[...]))
    grans = slots // GRAN
    slot_iota = iota((LANES, slots), 1).astype(F32)
    for sub in range(rows // BLOCK_ROWS):
        row0 = sub * BLOCK_ROWS
        y = ys_ref[sub * grans : (sub + 1) * grans].reshape(slots, ys_ref.shape[2])
        hot = [(slot_iota == pos_cols[:, r : r + 1]).astype(F32).astype(BF16) for r in range(row0, row0 + BLOCK_ROWS)]
        back = jnp.dot(jnp.concatenate(hot, axis=0), y, preferred_element_type=F32)
        for r in range(BLOCK_ROWS):
            at = (row0 + r) * LANES
            scaled = back[r * LANES : (r + 1) * LANES] * gate_cols[:, row0 + r : row0 + r + 1]
            out_ref[at : at + LANES, :] = scaled.astype(BF16)


def vmem():
    return pl.BlockSpec(memory_space=pltpu.VMEM)


def smem():
    return pl.BlockSpec(memory_space=pltpu.SMEM)


def hbm():
    return pl.BlockSpec(memory_space=pl.ANY)


def solution(mesh):
    num_experts = mesh.shape["ep_b"] * mesh.shape["ep_a"]
    tok_spec = P(("dp",) + EXPERT_AXES)
    expert_spec = P(EXPERT_AXES)

    def swap(value, bit):
        return lax.ppermute(value, EXPERT_AXES, [(e, e ^ bit) for e in range(num_experts)])

    def inner_step(tokens, expert_ids, route_order, w_route, expert_keys, value_a11, w_in, b_in, w_out, b_out):
        tok_dev, width = tokens.shape[1], tokens.shape[2]
        hidden = w_in.shape[2]
        router = w_route.shape[1]
        capacity = (5 * tok_dev + 4 * num_experts - 1) // (4 * num_experts)
        rows = tok_dev // LANES
        blocks = rows // BLOCK_ROWS
        slots = -(-(BLOCK_ROWS * LANES + num_experts * (GRAN - 1)) // LANES) * LANES
        span = slots // GRAN
        me = lax.axis_index(EXPERT_AXES)

        first, second = w_in[0], w_out[0]
        x_first, y_second = swap(first, 2), swap(second, 4)
        x_second, y_first = swap(second, 2), swap(first, 4)
        c_first, c_second = swap(first, 1), swap(second, 1)
        own_bias = jnp.concatenate([b_in, b_out], axis=1)
        bias = [own_bias] + [swap(own_bias, bit) for bit in range(1, num_experts)]

        ids, order = expert_ids.reshape(rows, LANES), route_order.reshape(rows, LANES)
        unit = 2 * BLOCK_ROWS
        whole = pl.BlockSpec((rows, LANES), lambda i: (0, 0))
        table = pl.BlockSpec((blocks, LANES), lambda i: (0, 0))
        pos, starts, counts, gate, xs = pl.pallas_call(
            functools.partial(dispatch_kernel, router, num_experts, capacity, slots),
            out_shape=(
                jax.ShapeDtypeStruct((rows, LANES), jnp.int32),
                jax.ShapeDtypeStruct((blocks, LANES), jnp.int32),
                jax.ShapeDtypeStruct((blocks, LANES), jnp.int32),
                jax.ShapeDtypeStruct((rows, LANES), F32),
                jax.ShapeDtypeStruct((blocks * span, GRAN, width), BF16),
            ),
            grid=(rows // unit,),
            in_specs=[
                smem(),
                whole,
                whole,
                pl.BlockSpec((width, router), lambda i: (0, 0)),
                pl.BlockSpec((num_experts, router), lambda i: (0, 0)),
                pl.BlockSpec((unit * LANES, width), lambda i: (i, 0)),
            ],
            out_specs=(
                whole,
                table,
                table,
                pl.BlockSpec((unit, LANES), lambda i: (i, 0)),
                pl.BlockSpec((2 * span, GRAN, width), lambda i: (i, 0, 0)),
            ),
            scratch_shapes=[pltpu.VMEM((router + 4 * num_experts, width), BF16)],
            cost_estimate=pl.CostEstimate(flops=9 * 10**9, bytes_accessed=14 * 10**6, transcendentals=0),
            name="dispatch",
        )(value_a11.reshape(1, 1), ids, order, w_route, expert_keys, tokens[0])

        most = -(-(capacity + blocks * (GRAN - 1)) // (16 * GRAN)) * 16
        tile, window = 16, 8

        def eids(bits):
            return jnp.stack([me ^ bits, me ^ bits ^ 1]).reshape(1, 2).astype(jnp.int32)

        def scratch(n, extra):
            return [
                pltpu.VMEM((n,) + first.shape, BF16),
                pltpu.VMEM((n,) + second.shape, BF16),
                pltpu.VMEM((n, most + extra, GRAN, width), BF16),
                pltpu.VMEM((tile * GRAN, hidden), BF16),
                pltpu.SemaphoreType.DMA((2 * n,)),
                pltpu.SemaphoreType.DMA((n,)),
            ]

        def eids(*bits):
            return jnp.stack([me ^ bit for bit in bits]).reshape(1, len(bits)).astype(jnp.int32)

        def experts(bits, xs, firsts, seconds):
            n = len(bits)
            return pl.pallas_call(
                functools.partial(expert_kernel, n, tile, span),
                out_shape=jax.ShapeDtypeStruct(xs.shape, BF16),
                in_specs=[smem()] * 3 + [hbm()] * (1 + 2 * n) + [vmem()] * n,
                out_specs=hbm(),
                scratch_shapes=scratch(n, 0) + [pltpu.SemaphoreType.DMA((n,))],
                input_output_aliases={3: 0},
                cost_estimate=pl.CostEstimate(flops=3 * n * 10**9, bytes_accessed=4 * n * 10**6, transcendentals=0),
            )(eids(*bits), starts, counts, xs, *firsts, *seconds, *[bias[bit] for bit in bits])

        xs = experts((0, 1), xs, (first, c_first), (second, c_second))
        x_first, y_second, xs = lax.optimization_barrier((x_first, y_second, xs))
        d_first, d_second = swap(x_first, 4), swap(y_second, 2)
        cx_first, cy_second = swap(x_first, 1), swap(y_second, 1)
        cx_second, cy_first = swap(x_second, 1), swap(y_first, 1)
        xs = experts((2, 3, 4, 5), xs, (x_first, cx_first, y_first, cy_first), (x_second, cx_second, y_second, cy_second))
        part = pl.pallas_call(
            functools.partial(combine_kernel, slots),
            out_shape=jax.ShapeDtypeStruct((tok_dev, width), BF16),
            grid=(rows // unit,),
            in_specs=[
                smem(),
                pl.BlockSpec((2 * span, GRAN, width), lambda i: (i, 0, 0)),
                pl.BlockSpec((unit, LANES), lambda i: (i, 0)),
                pl.BlockSpec((unit, LANES), lambda i: (i, 0)),
                pl.BlockSpec((unit, LANES), lambda i: (i, 0)),
            ],
            out_specs=pl.BlockSpec((unit * LANES, width), lambda i: (i, 0)),
            cost_estimate=pl.CostEstimate(flops=5 * 10**9, bytes_accessed=14 * 10**6, transcendentals=0),
            name="combine",
        )(eids(6, 7), xs, pos, gate, ids)
        d_first, d_second, part = lax.optimization_barrier((d_first, d_second, part))
        out = pl.pallas_call(
            functools.partial(final_kernel, 2, tile, span, window),
            out_shape=jax.ShapeDtypeStruct((tok_dev, width), BF16),
            in_specs=[smem()] * 3 + [vmem()] * 3 + [hbm()] * 6 + [vmem()] * 2,
            out_specs=hbm(),
            scratch_shapes=scratch(2, tile + window)
            + [pltpu.VMEM((tok_dev, width), BF16), pltpu.SemaphoreType.DMA, pltpu.SemaphoreType.DMA],
            cost_estimate=pl.CostEstimate(flops=7 * 10**9, bytes_accessed=8 * 10**6, transcendentals=0),
            name="final",
        )(
            eids(6, 7), starts, counts, pos, gate, ids, xs, part,
            d_first, swap(d_first, 1), d_second, swap(d_second, 1), bias[6], bias[7],
        )
        return out[None]

    return jax.shard_map(
        inner_step,
        mesh=mesh,
        in_specs=(tok_spec, tok_spec, tok_spec, P(), P(), P(), expert_spec, expert_spec, expert_spec, expert_spec),
        out_specs=tok_spec,
        check_vma=False,
    )
```

```python
import functools

import jax
import jax.numpy as jnp
from jax import lax
from jax.experimental import pallas as pl
from jax.experimental.pallas import tpu as pltpu
from jax.sharding import PartitionSpec as P


EXPERT_AXES = ("ep_b", "ep_a")

LANES = 128
BLOCK_ROWS = 4
GRAN = 16
BF16 = jnp.bfloat16
F32 = jnp.float32
NT = (((1,), (1,)), ((), ()))


def iota(shape, dim):
    return lax.broadcasted_iota(jnp.int32, shape, dim)


def plan_step(num_experts, capacity, span, ids_ref, ord_ref, wr_ref, keys_ref, pos_ref, start_ref, count_ref, offset_ref, list_ref, wt_ref):
    rows = ids_ref.shape[0]
    blocks = rows // BLOCK_ROWS
    place = jnp.zeros((2 * rows, LANES), F32)
    hi_iota = iota((rows, LANES), 0)
    lo_iota = iota((LANES, LANES), 0)
    lane_val = iota((rows, LANES), 1).astype(F32)
    for chunk in range(rows // 8):
        left, right = [], []
        for r in range(8 * chunk, 8 * chunk + 8):
            order_row = ord_ref[r : r + 1, :]
            hit = hi_iota == (order_row >> 7)
            upper = jnp.where(hit, F32(r), 0.0).astype(BF16)
            lower = jnp.where(hit, lane_val, 0.0).astype(BF16)
            left.append(jnp.concatenate([upper, lower], axis=0))
            right.append(jnp.where(lo_iota == (order_row & 127), 1.0, 0.0).astype(BF16))
        place += lax.dot_general(jnp.concatenate(left, axis=1), jnp.concatenate(right, axis=1), NT, preferred_element_type=F32)
    place = (place[:rows] * LANES + place[rows:]).astype(jnp.int32)
    ids = ids_ref[...]
    mask = (ids[None] == iota((num_experts, rows, LANES), 0)).astype(F32)

    def narrow(step, bound):
        trial = bound + (2 * rows * LANES >> (step + 1))
        admitted = jnp.where(place[None] < trial, mask, 0.0)
        total = jnp.sum(jnp.sum(admitted, axis=1, keepdims=True), axis=2, keepdims=True)
        return jnp.where(total <= capacity, trial, bound)

    steps = (rows * LANES).bit_length()
    bound = lax.fori_loop(0, steps, narrow, jnp.zeros((num_experts, 1, 1), jnp.int32))
    kept = jnp.where(place[None] < bound, mask, 0.0)
    kept2 = kept.reshape(num_experts * rows, LANES).astype(BF16)
    before = (iota((LANES, LANES), 0) < iota((LANES, LANES), 1)).astype(BF16)
    lane_prefix = jnp.dot(kept2, before, preferred_element_type=F32)
    row_total = jnp.dot(kept2, jnp.ones((LANES, LANES), BF16), preferred_element_type=F32).astype(BF16)
    row_a, row_b = iota((rows, rows), 0), iota((rows, rows), 1)
    same = row_a // BLOCK_ROWS == row_b // BLOCK_ROWS
    earlier = (same & (row_b < row_a)).astype(BF16)
    same = same.astype(BF16)
    pick = (iota((blocks, rows), 1) == iota((blocks, rows), 0) * BLOCK_ROWS).astype(BF16)
    lane = iota((blocks, LANES), 1)
    slot = jnp.full((rows, LANES), -1, jnp.int32)
    first = jnp.zeros((rows, LANES), jnp.int32)
    starts = jnp.zeros((blocks, LANES), F32)
    counts = jnp.zeros((blocks, LANES), F32)
    offsets = jnp.zeros((blocks, LANES), F32)
    block_iota = iota((blocks, LANES), 0)
    past = (iota((blocks, blocks), 1) < iota((blocks, blocks), 0)).astype(BF16)
    for e in range(num_experts):
        part = slice(e * rows, (e + 1) * rows)
        row_prefix = jnp.dot(earlier, row_total[part], preferred_element_type=F32)
        in_block = jnp.dot(same, row_total[part], preferred_element_type=F32).astype(jnp.int32)
        grans = (in_block + (GRAN - 1)) >> 4
        here = first * GRAN + (row_prefix + lane_prefix[part]).astype(jnp.int32)
        slot = jnp.where(kept[e] > 0.0, here, slot)
        first_b = jnp.dot(pick, first.astype(F32).astype(BF16), preferred_element_type=F32)
        count_b = jnp.dot(pick, grans.astype(F32).astype(BF16), preferred_element_type=F32)
        offset_b = jnp.dot(past, count_b.astype(BF16), preferred_element_type=F32)
        starts += jnp.where(lane == e, first_b, 0.0)
        counts += jnp.where(lane == e, count_b, 0.0)
        offsets += jnp.where(lane == e, offset_b, 0.0)
        index = (lane - offset_b.astype(jnp.int32) + first_b.astype(jnp.int32) + block_iota * span).astype(F32)
        inside = (lane.astype(F32) >= offset_b) & (lane.astype(F32) < offset_b + count_b)
        index = jnp.sum(jnp.where(inside, index - blocks * span, 0.0), axis=0, keepdims=True)
        list_ref[e : e + 1, :] = index.astype(jnp.int32) + blocks * span
        first = first + grans
    pos_ref[...] = slot
    start_ref[...] = starts.astype(jnp.int32)
    offset_ref[...] = offsets.astype(jnp.int32)
    count_ref[...] = counts.astype(jnp.int32)
    wr = wr_ref[...]
    router = wr.shape[1]
    eye = (iota((router, router), 0) == iota((router, router), 1)).astype(BF16)
    keys = keys_ref[...].astype(F32)
    unit = keys / jnp.sqrt(jnp.sum(keys * keys, axis=1, keepdims=True))
    folded = lax.dot_general(unit, wr.astype(F32), NT, preferred_element_type=F32, precision=lax.Precision.HIGHEST)
    part_a = folded.astype(BF16)
    rest = folded - part_a.astype(F32)
    part_b = rest.astype(BF16)
    part_c = (rest - part_b.astype(F32)).astype(BF16)
    wt_ref[0:router, :] = lax.dot_general(eye, wr, NT, preferred_element_type=F32).astype(BF16)
    tail = jnp.concatenate([part_a.astype(F32), part_b.astype(F32), part_c.astype(F32), jnp.zeros_like(folded)], axis=0)
    wt_ref[router:, :] = tail.astype(BF16)


def dispatch_kernel(
    router, num_experts, capacity, slots, tau_ref, ids_ref, ord_ref, wr_ref, keys_ref, x_ref,
    pos_ref, start_ref, count_ref, offset_ref, list_ref, gate_ref, xs_ref, wt_ref,
):
    grans = slots // GRAN
    spare = start_ref.shape[0] * grans

    @pl.when(pl.program_id(0) == 0)
    def _():
        plan_step(
            num_experts, capacity, grans, ids_ref, ord_ref, wr_ref, keys_ref,
            pos_ref, start_ref, count_ref, offset_ref, list_ref, wt_ref,
        )
        xs_ref[spare : spare + 2] = jnp.zeros((2,) + xs_ref.shape[1:], BF16)

    rows = x_ref.shape[0] // LANES
    part = pl.ds(pl.multiple_of(pl.program_id(0) * rows, rows), rows)
    ids, pos = ids_ref[part, :], pos_ref[part, :]
    tau = tau_ref[0, 0]
    for sub in range(rows // BLOCK_ROWS):
        row0 = sub * BLOCK_ROWS
        x = x_ref[row0 * LANES : (row0 + BLOCK_ROWS) * LANES, :]
        proj = lax.dot_general(wt_ref[...], x, NT, preferred_element_type=F32)
        square = jnp.sum(proj[:router] * proj[:router], axis=0, keepdims=True)
        ne = num_experts
        logits = proj[router : router + ne] + proj[router + ne : router + 2 * ne] + proj[router + 2 * ne : router + 3 * ne]
        logits = logits / jnp.sqrt(square) / tau
        expo = jnp.exp(logits - jnp.max(logits, axis=0, keepdims=True))
        prob = expo / jnp.sum(expo, axis=0, keepdims=True)
        id_row = jnp.concatenate([ids[r : r + 1] for r in range(row0, row0 + BLOCK_ROWS)], axis=1)
        gate = jnp.sum(jnp.where(iota(prob.shape, 0) == id_row, prob, 0.0), axis=0, keepdims=True)
        for r in range(BLOCK_ROWS):
            gate_ref[row0 + r : row0 + r + 1, :] = gate[:, r * LANES : (r + 1) * LANES]
        slot_iota = iota((slots, LANES), 0)
        hot = [(slot_iota == pos[r : r + 1]).astype(F32).astype(BF16) for r in range(row0, row0 + BLOCK_ROWS)]
        picked = jnp.dot(jnp.concatenate(hot, axis=1), x, preferred_element_type=F32).astype(BF16)
        at = pl.ds((pl.program_id(0) * (rows // BLOCK_ROWS) + sub) * grans, grans)
        xs_ref[at] = picked.reshape(grans, GRAN, picked.shape[1])


def expert_names(bits):
    me = lax.axis_index("ep_b") * lax.axis_size("ep_a") + lax.axis_index("ep_a")
    return [me ^ bit for bit in bits]


def run_expert(e, tile, list_ref, start_count, b_ref, w1_ref, w2_ref, xs_ref, h_buf, put):
    width, hidden = w1_ref.shape
    total = start_count
    b1 = b_ref[:, 0:hidden].astype(F32)
    b2 = b_ref[:, hidden : hidden + width].astype(F32)

    def per_tile(t, _):
        names = [list_ref[e, t * tile + k] for k in range(tile)]
        x = jnp.concatenate([xs_ref[name] for name in names], axis=0)
        step = 256
        for c in range(0, hidden, step):
            pre = jnp.dot(x, w1_ref[:, c : c + step], preferred_element_type=F32) + b1[:, c : c + step]
            act = 0.5 * pre * (1.0 + lax.erf(pre * F32(0.5**0.5)))
            h_buf[:, c : c + step] = act.astype(BF16)
        y = jnp.dot(h_buf[...], w2_ref[...], preferred_element_type=F32) + b2
        put(t, names, y.astype(BF16))
        return 0

    lax.fori_loop(0, (total + tile - 1) // tile, per_tile, 0)


def expert_kernel(bits, tile, spare, count_ref, offset_ref, list_ref, xs_ref, *refs):
    count, experts = len(bits), expert_names(bits)
    w1_refs, w2_refs, b_refs = refs[:count], refs[count : 2 * count], refs[2 * count : 3 * count]
    out_ref, h_buf = refs[3 * count :]
    last = count_ref.shape[0] - 1

    def put(t, names, y):
        for k, name in enumerate(names):
            out_ref[jnp.where(name == spare, spare + 1, name)] = y[k * GRAN : (k + 1) * GRAN]

    for i in range(count):
        e = experts[i]
        run_expert(e, tile, list_ref, offset_ref[last, e] + count_ref[last, e], b_refs[i], w1_refs[i], w2_refs[i], xs_ref, h_buf, put)


def final_kernel(
    bits, tile, window, start_ref, count_ref, offset_ref, list_ref, pos_ref, gate_ref, ids_ref, xs_ref, part_ref, *refs
):
    count, experts = len(bits), expert_names(bits)
    w1_refs, w2_refs, b_refs = refs[:count], refs[count : 2 * count], refs[2 * count : 3 * count]
    out_ref, h_buf, y_buf, o_buf, o_sem = refs[3 * count :]
    blocks = start_ref.shape[0]
    width = w1_refs[0].shape[0]
    block_tok = BLOCK_ROWS * LANES
    totals = [offset_ref[blocks - 1, experts[i]] + count_ref[blocks - 1, experts[i]] for i in range(count)]
    for i in range(count):

        def put(t, names, y):
            y_buf[i, pl.ds(t * tile, tile)] = y.reshape(tile, GRAN, width)

        run_expert(experts[i], tile, list_ref, totals[i], b_refs[i], w1_refs[i], w2_refs[i], xs_ref, h_buf, put)
        y_buf[i, pl.ds((totals[i] + tile - 1) // tile * tile, window)] = jnp.zeros((window, GRAN, width), BF16)
    lane = iota((LANES, window * GRAN), 1).astype(F32)

    def out_copy(pair, slot):
        rows = pl.ds(pl.multiple_of(pair * 2 * block_tok, 2 * block_tok), 2 * block_tok)
        return pltpu.make_async_copy(o_buf.at[slot], out_ref.at[rows], o_sem.at[slot])

    def per_pair(pair, _):
        slot = pair % 2
        row0 = pl.multiple_of(pair * 2 * BLOCK_ROWS, 2 * BLOCK_ROWS)
        rows8 = pl.ds(row0, 2 * BLOCK_ROWS)
        pos8, gate8, ids8 = pos_ref[rows8, :], gate_ref[rows8, :], ids_ref[rows8, :]
        gate_cols = jnp.transpose(gate8)
        upper = iota(pos8.shape, 0) < BLOCK_ROWS
        local = []
        for i in range(count):
            e = experts[i]
            origin = jnp.where(upper, start_ref[2 * pair, e], start_ref[2 * pair + 1, e]) * GRAN
            mine = (ids8 == e) & (pos8 >= 0)
            local.append(jnp.transpose(jnp.where(mine, pos8 - origin, -1).astype(F32)))

        def window_rows(sub, w, offsets):
            ys = jnp.concatenate(
                [y_buf[i, pl.ds(jnp.minimum(offsets[i] + w * window, totals[i]), window)].reshape(window * GRAN, width) for i in range(count)],
                axis=0,
            )
            shift = jnp.asarray(w * (window * GRAN)).astype(F32)
            hot = []
            for r in range(sub * BLOCK_ROWS, (sub + 1) * BLOCK_ROWS):
                hot.append(jnp.concatenate([(lane == local[i][:, r : r + 1] - shift).astype(F32).astype(BF16) for i in range(count)], axis=1))
            return jnp.dot(jnp.concatenate(hot, axis=0), ys, preferred_element_type=F32)

        def scaled(sub, back, r):
            return back[r * LANES : (r + 1) * LANES] * gate_cols[:, sub * BLOCK_ROWS + r : sub * BLOCK_ROWS + r + 1]

        @pl.when(pair >= 2)
        def _():
            out_copy(pair, slot).wait()

        for sub in range(2):
            b = 2 * pair + sub
            sizes = [count_ref[b, experts[i]] for i in range(count)]
            starts = [offset_ref[b, experts[i]] for i in range(count)]
            back = window_rows(sub, 0, starts)
            for r in range(BLOCK_ROWS):
                source = pl.ds(pl.multiple_of(b * block_tok + r * LANES, LANES), LANES)
                at = slice((sub * BLOCK_ROWS + r) * LANES, (sub * BLOCK_ROWS + r + 1) * LANES)
                o_buf[slot, at, :] = (part_ref[source, :].astype(F32) + scaled(sub, back, r)).astype(BF16)

        for sub in range(2):
            b = 2 * pair + sub
            sizes = [count_ref[b, experts[i]] for i in range(count)]
            starts = [offset_ref[b, experts[i]] for i in range(count)]
            longest = sizes[0]
            for size in sizes[1:]:
                longest = jnp.maximum(longest, size)

            def more(w, _):
                back = window_rows(sub, w, starts)
                for r in range(BLOCK_ROWS):
                    at = slice((sub * BLOCK_ROWS + r) * LANES, (sub * BLOCK_ROWS + r + 1) * LANES)
                    o_buf[slot, at, :] = (o_buf[slot, at, :].astype(F32) + scaled(sub, back, r)).astype(BF16)
                return 0

            lax.fori_loop(1, (longest + window - 1) // window, more, 0)
        out_copy(pair, slot).start()
        return 0

    lax.fori_loop(0, blocks // 2, per_pair, 0)
    for slot in range(2):
        out_copy(0, slot).wait()


def combine_kernel(slots, bits, ys_ref, pos_ref, gate_ref, ids_ref, out_ref):
    experts = expert_names(bits)
    rows = pos_ref.shape[0]
    pos_cols = jnp.transpose(pos_ref[...].astype(F32))
    later = (ids_ref[...] == experts[0]) | (ids_ref[...] == experts[1])
    gate_cols = jnp.transpose(jnp.where(later, 0.0, gate_ref[...]))
    grans = slots // GRAN
    slot_iota = iota((LANES, slots), 1).astype(F32)
    for sub in range(rows // BLOCK_ROWS):
        row0 = sub * BLOCK_ROWS
        y = ys_ref[pl.ds((pl.program_id(0) * (rows // BLOCK_ROWS) + sub) * grans, grans)].reshape(slots, ys_ref.shape[2])
        hot = [(slot_iota == pos_cols[:, r : r + 1]).astype(F32).astype(BF16) for r in range(row0, row0 + BLOCK_ROWS)]
        back = jnp.dot(jnp.concatenate(hot, axis=0), y, preferred_element_type=F32)
        for r in range(BLOCK_ROWS):
            at = pl.ds(pl.multiple_of(((pl.program_id(0) * rows) + row0 + r) * LANES, LANES), LANES)
            scaled = back[r * LANES : (r + 1) * LANES] * gate_cols[:, row0 + r : row0 + r + 1]
            out_ref[at, :] = scaled.astype(BF16)


def vmem():
    return pl.BlockSpec(memory_space=pltpu.VMEM)


def smem():
    return pl.BlockSpec(memory_space=pltpu.SMEM)


def hbm():
    return pl.BlockSpec(memory_space=pl.ANY)


def solution(mesh):
    num_experts = mesh.shape["ep_b"] * mesh.shape["ep_a"]
    tok_spec = P(("dp",) + EXPERT_AXES)
    expert_spec = P(EXPERT_AXES)

    def swap(value, bit):
        return lax.ppermute(value, EXPERT_AXES, [(e, e ^ bit) for e in range(num_experts)])

    def inner_step(tokens, expert_ids, route_order, w_route, expert_keys, value_a11, w_in, b_in, w_out, b_out):
        tok_dev, width = tokens.shape[1], tokens.shape[2]
        hidden = w_in.shape[2]
        router = w_route.shape[1]
        capacity = (5 * tok_dev + 4 * num_experts - 1) // (4 * num_experts)
        rows = tok_dev // LANES
        blocks = rows // BLOCK_ROWS
        slots = -(-(BLOCK_ROWS * LANES + num_experts * (GRAN - 1)) // LANES) * LANES
        span = slots // GRAN

        first, second = w_in[0], w_out[0]
        x_first, y_second = swap(first, 2), swap(second, 4)
        x_second, y_first = swap(second, 2), swap(first, 4)
        c_first, c_second = swap(first, 1), swap(second, 1)
        own_bias = jnp.concatenate([b_in, b_out], axis=1)
        bias = [own_bias] + [swap(own_bias, bit) for bit in range(1, num_experts)]

        ids, order = expert_ids.reshape(rows, LANES), route_order.reshape(rows, LANES)
        unit = 2 * BLOCK_ROWS
        small = functools.partial(pl.BlockSpec, index_map=lambda i: (0, 0))
        whole = small((rows, LANES))
        table = small((blocks, LANES))
        xs_shape = (blocks * span + 8, GRAN, width)
        pos, starts, counts, offsets, lists, gate, xs = pl.pallas_call(
            functools.partial(dispatch_kernel, router, num_experts, capacity, slots),
            out_shape=(
                jax.ShapeDtypeStruct((rows, LANES), jnp.int32),
                jax.ShapeDtypeStruct((blocks, LANES), jnp.int32),
                jax.ShapeDtypeStruct((blocks, LANES), jnp.int32),
                jax.ShapeDtypeStruct((blocks, LANES), jnp.int32),
                jax.ShapeDtypeStruct((num_experts, LANES), jnp.int32),
                jax.ShapeDtypeStruct((rows, LANES), F32),
                pltpu.VMEM(xs_shape, BF16),
            ),
            grid=(rows // unit,),
            in_specs=[
                smem(),
                whole,
                whole,
                small((width, router)),
                small((num_experts, router)),
                pl.BlockSpec((unit * LANES, width), lambda i: (i, 0)),
            ],
            out_specs=(
                whole,
                table,
                table,
                table,
                small((num_experts, LANES)),
                pl.BlockSpec((unit, LANES), lambda i: (i, 0)),
                vmem(),
            ),
            scratch_shapes=[pltpu.VMEM((router + 4 * num_experts, width), BF16)],
            cost_estimate=pl.CostEstimate(flops=9 * 10**9, bytes_accessed=14 * 10**6, transcendentals=0),
            compiler_params=pltpu.CompilerParams(vmem_limit_bytes=12 * 2**20),
            name="dispatch",
        )(value_a11.reshape(1, 1), ids, order, w_route, expert_keys, tokens[0])

        most = -(-(capacity + blocks * (GRAN - 1)) // (16 * GRAN)) * 16
        tile, window = 16, 8
        held = lambda array: pltpu.with_memory_space_constraint(array, pltpu.VMEM)

        def experts(bits, xs, firsts, seconds):
            n = len(bits)
            return pl.pallas_call(
                functools.partial(expert_kernel, bits, tile, blocks * span),
                out_shape=pltpu.VMEM(xs.shape, BF16),
                in_specs=[smem()] * 3 + [vmem()] * (1 + 3 * n),
                out_specs=vmem(),
                scratch_shapes=[pltpu.VMEM((tile * GRAN, hidden), BF16)],
                input_output_aliases={3: 0},
                cost_estimate=pl.CostEstimate(flops=3 * n * 10**9, bytes_accessed=4 * n * 10**6, transcendentals=0),
                compiler_params=pltpu.CompilerParams(vmem_limit_bytes=8 * 2**20),
            )(counts, offsets, lists, held(xs), *map(held, firsts), *map(held, seconds), *[bias[bit] for bit in bits])

        xs = experts((0, 1), xs, (first, c_first), (second, c_second))
        x_first, y_second, xs = lax.optimization_barrier((x_first, y_second, xs))
        d_first, d_second = swap(x_first, 4), swap(y_second, 2)
        cx_first, cy_second = swap(x_first, 1), swap(y_second, 1)
        cx_second, cy_first = swap(x_second, 1), swap(y_first, 1)
        xs = experts((2, 3, 4, 5), xs, (x_first, cx_first, y_first, cy_first), (x_second, cx_second, y_second, cy_second))
        part = pl.pallas_call(
            functools.partial(combine_kernel, slots, (6, 7)),
            out_shape=pltpu.VMEM((tok_dev, width), BF16),
            grid=(rows // unit,),
            in_specs=[
                vmem(),
                pl.BlockSpec((unit, LANES), lambda i: (i, 0)),
                pl.BlockSpec((unit, LANES), lambda i: (i, 0)),
                pl.BlockSpec((unit, LANES), lambda i: (i, 0)),
            ],
            out_specs=vmem(),
            cost_estimate=pl.CostEstimate(flops=5 * 10**9, bytes_accessed=14 * 10**6, transcendentals=0),
            compiler_params=pltpu.CompilerParams(vmem_limit_bytes=8 * 2**20),
            name="combine",
        )(held(xs), pos, gate, ids)
        d_first, d_second, part = lax.optimization_barrier((d_first, d_second, part))
        firsts = (d_first, swap(d_first, 1))
        seconds = (d_second, swap(d_second, 1))
        out = pl.pallas_call(
            functools.partial(final_kernel, (6, 7), tile, window),
            out_shape=jax.ShapeDtypeStruct((tok_dev, width), BF16),
            in_specs=[smem()] * 4 + [vmem()] * (5 + 6),
            out_specs=hbm(),
            scratch_shapes=[
                pltpu.VMEM((tile * GRAN, hidden), BF16),
                pltpu.VMEM((2, most + tile, GRAN, width), BF16),
                pltpu.VMEM((2, 2 * BLOCK_ROWS * LANES, width), BF16),
                pltpu.SemaphoreType.DMA((2,)),
            ],
            cost_estimate=pl.CostEstimate(flops=7 * 10**9, bytes_accessed=8 * 10**6, transcendentals=0),
            compiler_params=pltpu.CompilerParams(vmem_limit_bytes=12 * 2**20),
            name="final",
        )(
            starts, counts, offsets, lists, pos, gate, ids, held(xs), held(part),
            *map(held, firsts), *map(held, seconds), bias[6], bias[7],
        )
        return out[None]

    return jax.shard_map(
        inner_step,
        mesh=mesh,
        in_specs=(tok_spec, tok_spec, tok_spec, P(), P(), P(), expert_spec, expert_spec, expert_spec, expert_spec),
        out_specs=tok_spec,
        check_vma=False,
    )
```

```python
import functools

import jax
import jax.numpy as jnp
from jax import lax
from jax.experimental import pallas as pl
from jax.experimental.pallas import tpu as pltpu
from jax.sharding import PartitionSpec as P


EXPERT_AXES = ("ep_b", "ep_a")

LANES = 128
BLOCK_ROWS = 4
GRAN = 16
BF16 = jnp.bfloat16
F32 = jnp.float32
NT = (((1,), (1,)), ((), ()))


def iota(shape, dim):
    return lax.broadcasted_iota(jnp.int32, shape, dim)


def plan_step(num_experts, capacity, span, ids_ref, ord_ref, wr_ref, keys_ref, pos_ref, start_ref, count_ref, offset_ref, list_ref, wt_ref):
    rows = ids_ref.shape[0]
    blocks = rows // BLOCK_ROWS
    place = jnp.zeros((2 * rows, LANES), F32)
    hi_iota = iota((rows, LANES), 0)
    lo_iota = iota((LANES, LANES), 0)
    lane_val = iota((rows, LANES), 1).astype(F32)
    for chunk in range(rows // 8):
        left, right = [], []
        for r in range(8 * chunk, 8 * chunk + 8):
            order_row = ord_ref[r : r + 1, :]
            hit = hi_iota == (order_row >> 7)
            upper = jnp.where(hit, F32(r), 0.0).astype(BF16)
            lower = jnp.where(hit, lane_val, 0.0).astype(BF16)
            left.append(jnp.concatenate([upper, lower], axis=0))
            right.append(jnp.where(lo_iota == (order_row & 127), 1.0, 0.0).astype(BF16))
        place += lax.dot_general(jnp.concatenate(left, axis=1), jnp.concatenate(right, axis=1), NT, preferred_element_type=F32)
    place = (place[:rows] * LANES + place[rows:]).astype(jnp.int32)
    ids = ids_ref[...]
    mask = (ids[None] == iota((num_experts, rows, LANES), 0)).astype(F32)

    def narrow(step, bound):
        trial = bound + (2 * rows * LANES >> (step + 1))
        admitted = jnp.where(place[None] < trial, mask, 0.0)
        total = jnp.sum(jnp.sum(admitted, axis=1, keepdims=True), axis=2, keepdims=True)
        return jnp.where(total <= capacity, trial, bound)

    steps = (rows * LANES).bit_length()
    bound = lax.fori_loop(0, steps, narrow, jnp.zeros((num_experts, 1, 1), jnp.int32))
    kept = jnp.where(place[None] < bound, mask, 0.0)
    kept2 = kept.reshape(num_experts * rows, LANES).astype(BF16)
    before = (iota((LANES, LANES), 0) < iota((LANES, LANES), 1)).astype(BF16)
    lane_prefix = jnp.dot(kept2, before, preferred_element_type=F32)
    row_total = jnp.dot(kept2, jnp.ones((LANES, LANES), BF16), preferred_element_type=F32).astype(BF16)
    row_a, row_b = iota((rows, rows), 0), iota((rows, rows), 1)
    same = row_a // BLOCK_ROWS == row_b // BLOCK_ROWS
    earlier = (same & (row_b < row_a)).astype(BF16)
    same = same.astype(BF16)
    pick = (iota((blocks, rows), 1) == iota((blocks, rows), 0) * BLOCK_ROWS).astype(BF16)
    lane = iota((blocks, LANES), 1)
    slot = jnp.full((rows, LANES), -1, jnp.int32)
    first = jnp.zeros((rows, LANES), jnp.int32)
    starts = jnp.zeros((blocks, LANES), F32)
    counts = jnp.zeros((blocks, LANES), F32)
    offsets = jnp.zeros((blocks, LANES), F32)
    block_iota = iota((blocks, LANES), 0)
    past = (iota((blocks, blocks), 1) < iota((blocks, blocks), 0)).astype(BF16)
    for e in range(num_experts):
        part = slice(e * rows, (e + 1) * rows)
        row_prefix = jnp.dot(earlier, row_total[part], preferred_element_type=F32)
        in_block = jnp.dot(same, row_total[part], preferred_element_type=F32).astype(jnp.int32)
        grans = (in_block + (GRAN - 1)) >> 4
        here = first * GRAN + (row_prefix + lane_prefix[part]).astype(jnp.int32)
        slot = jnp.where(kept[e] > 0.0, here, slot)
        first_b = jnp.dot(pick, first.astype(F32).astype(BF16), preferred_element_type=F32)
        count_b = jnp.dot(pick, grans.astype(F32).astype(BF16), preferred_element_type=F32)
        offset_b = jnp.dot(past, count_b.astype(BF16), preferred_element_type=F32)
        starts += jnp.where(lane == e, first_b, 0.0)
        counts += jnp.where(lane == e, count_b, 0.0)
        offsets += jnp.where(lane == e, offset_b, 0.0)
        index = (lane - offset_b.astype(jnp.int32) + first_b.astype(jnp.int32) + block_iota * span).astype(F32)
        inside = (lane.astype(F32) >= offset_b) & (lane.astype(F32) < offset_b + count_b)
        index = jnp.sum(jnp.where(inside, index - blocks * span, 0.0), axis=0, keepdims=True)
        list_ref[e : e + 1, :] = index.astype(jnp.int32) + blocks * span
        first = first + grans
    pos_ref[...] = slot
    start_ref[...] = starts.astype(jnp.int32)
    offset_ref[...] = offsets.astype(jnp.int32)
    count_ref[...] = counts.astype(jnp.int32)
    wr = wr_ref[...]
    router = wr.shape[1]
    eye = (iota((router, router), 0) == iota((router, router), 1)).astype(BF16)
    keys = keys_ref[...].astype(F32)
    unit = keys / jnp.sqrt(jnp.sum(keys * keys, axis=1, keepdims=True))
    folded = lax.dot_general(unit, wr.astype(F32), NT, preferred_element_type=F32, precision=lax.Precision.HIGHEST)
    part_a = folded.astype(BF16)
    rest = folded - part_a.astype(F32)
    part_b = rest.astype(BF16)
    part_c = (rest - part_b.astype(F32)).astype(BF16)
    wt_ref[0:router, :] = lax.dot_general(eye, wr, NT, preferred_element_type=F32).astype(BF16)
    tail = jnp.concatenate([part_a.astype(F32), part_b.astype(F32), part_c.astype(F32), jnp.zeros_like(folded)], axis=0)
    wt_ref[router:, :] = tail.astype(BF16)


def dispatch_kernel(
    router, num_experts, capacity, slots, tau_ref, ids_ref, ord_ref, wr_ref, keys_ref, x_ref,
    pos_ref, start_ref, count_ref, offset_ref, list_ref, gate_ref, xs_ref, wt_ref,
):
    grans = slots // GRAN
    spare = start_ref.shape[0] * grans

    @pl.when(pl.program_id(0) == 0)
    def _():
        plan_step(
            num_experts, capacity, grans, ids_ref, ord_ref, wr_ref, keys_ref,
            pos_ref, start_ref, count_ref, offset_ref, list_ref, wt_ref,
        )
        xs_ref[spare : spare + 2] = jnp.zeros((2,) + xs_ref.shape[1:], BF16)

    rows = x_ref.shape[0] // LANES
    part = pl.ds(pl.multiple_of(pl.program_id(0) * rows, rows), rows)
    ids, pos = ids_ref[part, :], pos_ref[part, :]
    tau = tau_ref[0, 0]
    for sub in range(rows // BLOCK_ROWS):
        row0 = sub * BLOCK_ROWS
        x = x_ref[row0 * LANES : (row0 + BLOCK_ROWS) * LANES, :]
        proj = lax.dot_general(wt_ref[...], x, NT, preferred_element_type=F32)
        square = jnp.sum(proj[:router] * proj[:router], axis=0, keepdims=True)
        ne = num_experts
        logits = proj[router : router + ne] + proj[router + ne : router + 2 * ne] + proj[router + 2 * ne : router + 3 * ne]
        logits = logits / jnp.sqrt(square) / tau
        expo = jnp.exp(logits - jnp.max(logits, axis=0, keepdims=True))
        prob = expo / jnp.sum(expo, axis=0, keepdims=True)
        id_row = jnp.concatenate([ids[r : r + 1] for r in range(row0, row0 + BLOCK_ROWS)], axis=1)
        gate = jnp.sum(jnp.where(iota(prob.shape, 0) == id_row, prob, 0.0), axis=0, keepdims=True)
        for r in range(BLOCK_ROWS):
            gate_ref[row0 + r : row0 + r + 1, :] = gate[:, r * LANES : (r + 1) * LANES]
        slot_iota = iota((slots, LANES), 0)
        hot = [(slot_iota == pos[r : r + 1]).astype(F32).astype(BF16) for r in range(row0, row0 + BLOCK_ROWS)]
        picked = jnp.dot(jnp.concatenate(hot, axis=1), x, preferred_element_type=F32).astype(BF16)
        at = pl.ds((pl.program_id(0) * (rows // BLOCK_ROWS) + sub) * grans, grans)
        xs_ref[at] = picked.reshape(grans, GRAN, picked.shape[1])


def expert_names(bits):
    me = lax.axis_index("ep_b") * lax.axis_size("ep_a") + lax.axis_index("ep_a")
    return [me ^ bit for bit in bits]


def stacked_dot(left, refs, columns):
    total, at = None, 0
    for ref in refs:
        depth = ref.shape[0]
        part = jnp.dot(left[:, at : at + depth], ref[:, columns], preferred_element_type=F32)
        total = part if total is None else total + part
        at += depth
    return total


def split_bias(ref, hidden):
    return ref[:, 0:hidden].astype(F32), ref[:, hidden:].astype(F32)


def up_tile(x, refs, b1, h_ref, at):
    hidden = refs[0].shape[1]
    step = 256
    for c in range(0, hidden, step):
        pre = stacked_dot(x, refs, slice(c, c + step)) + b1[:, c : c + step]
        act = 0.5 * pre * (1.0 + lax.erf(pre * F32(0.5**0.5)))
        h_ref[at, c : c + step] = act.astype(BF16)


def granules(e, count_ref, offset_ref):
    last = count_ref.shape[0] - 1
    return offset_ref[last, e] + count_ref[last, e]


def tile_names(e, t, tile, list_ref):
    return [list_ref[e, t * tile + k] for k in range(tile)]


def put_rows(names, spare, y, out_ref):
    for k, name in enumerate(names):
        out_ref[jnp.where(name == spare, spare + 1, name)] = y[k * GRAN : (k + 1) * GRAN]


def expert_kernel(bits, tile, spare, count_ref, offset_ref, list_ref, xs_ref, *refs):
    count = len(bits)
    w1_refs, w2_refs, b_refs = refs[:count], refs[count : 2 * count], refs[2 * count : 3 * count]
    out_ref, h_buf = refs[3 * count :]
    hidden = h_buf.shape[1]
    for i, e in enumerate(expert_names(bits)):
        b1, b2 = split_bias(b_refs[i], hidden)

        def per_tile(t, _):
            names = tile_names(e, t, tile, list_ref)
            up_tile(jnp.concatenate([xs_ref[name] for name in names], axis=0), [w1_refs[i]], b1, h_buf, slice(None))
            y = stacked_dot(h_buf[...], [w2_refs[i]], slice(None)) + b2
            put_rows(names, spare, y.astype(BF16), out_ref)
            return 0

        lax.fori_loop(0, (granules(e, count_ref, offset_ref) + tile - 1) // tile, per_tile, 0)


def up_kernel(bits, pieces, tile, most, count_ref, offset_ref, list_ref, xs_ref, *refs):
    count = len(bits)
    w1_refs = [refs[i * pieces : (i + 1) * pieces] for i in range(count)]
    b_refs = refs[count * pieces : count * pieces + count]
    h_ref = refs[count * pieces + count]
    hidden = h_ref.shape[1]
    for i, e in enumerate(expert_names(bits)):
        b1, _ = split_bias(b_refs[i], hidden)

        def per_tile(t, _):
            names = tile_names(e, t, tile, list_ref)
            at = pl.ds(pl.multiple_of((i * most + t * tile) * GRAN, tile * GRAN), tile * GRAN)
            up_tile(jnp.concatenate([xs_ref[name] for name in names], axis=0), w1_refs[i], b1, h_ref, at)
            return 0

        lax.fori_loop(0, (granules(e, count_ref, offset_ref) + tile - 1) // tile, per_tile, 0)


def down_kernel(bits, first, tile, most, spare, count_ref, offset_ref, list_ref, xs_ref, h_ref, *refs):
    count = len(bits)
    w2_refs, b_refs, out_ref = refs[:count], refs[count : 2 * count], refs[2 * count]
    del xs_ref
    for i, e in enumerate(expert_names(bits)):
        _, b2 = split_bias(b_refs[i], h_ref.shape[1])

        def per_tile(t, _):
            names = tile_names(e, t, tile, list_ref)
            at = pl.ds(pl.multiple_of(((first + i) * most + t * tile) * GRAN, tile * GRAN), tile * GRAN)
            y = stacked_dot(h_ref[at, :], [w2_refs[i]], slice(None)) + b2
            put_rows(names, spare, y.astype(BF16), out_ref)
            return 0

        lax.fori_loop(0, (granules(e, count_ref, offset_ref) + tile - 1) // tile, per_tile, 0)


def compact_down(place, total, tile, most, window, w2_refs, b_ref, h_ref, y_ref):
    width = y_ref.shape[2]
    _, b2 = split_bias(b_ref, h_ref.shape[1])

    def per_tile(t, _):
        at = pl.ds(pl.multiple_of((place * most + t * tile) * GRAN, tile * GRAN), tile * GRAN)
        y = stacked_dot(h_ref[at, :], w2_refs, slice(None)) + b2
        y_ref[pl.ds(t * tile, tile)] = y.astype(BF16).reshape(tile, GRAN, width)
        return 0

    tiles = (total + tile - 1) // tile
    lax.fori_loop(0, tiles, per_tile, 0)
    y_ref[pl.ds(tiles * tile, window)] = jnp.zeros((window, GRAN, width), BF16)


def half_kernel(bits, tile, most, window, count_ref, offset_ref, h_ref, *refs):
    total = granules(expert_names(bits)[0], count_ref, offset_ref)
    compact_down(0, total, tile, most, window, refs[:-2], refs[-2], h_ref, refs[-1])


def final_kernel(
    bits, tile, most, window, start_ref, count_ref, offset_ref, pos_ref, gate_ref, ids_ref, hot_ref, h_ref, part_ref, y_ref, *refs
):
    count, experts = len(bits), expert_names(bits)
    out_ref, y_buf, o_buf, o_sem = refs[-4:]
    y_refs = (y_ref, y_buf)
    blocks = start_ref.shape[0]
    width = part_ref.shape[1]
    block_tok = BLOCK_ROWS * LANES
    totals = [granules(e, count_ref, offset_ref) for e in experts]
    compact_down(1, totals[1], tile, most, window, refs[:-5], refs[-5], h_ref, y_buf)

    def out_copy(pair, slot):
        rows = pl.ds(pl.multiple_of(pair * 2 * block_tok, 2 * block_tok), 2 * block_tok)
        return pltpu.make_async_copy(o_buf.at[slot], out_ref.at[rows], o_sem.at[slot])

    def per_pair(pair, _):
        slot = pair % 2
        row0 = pl.multiple_of(pair * 2 * BLOCK_ROWS, 2 * BLOCK_ROWS)
        rows8 = pl.ds(row0, 2 * BLOCK_ROWS)
        gate_cols = jnp.transpose(gate_ref[rows8, :])

        def window_rows(sub, w, hot):
            ys = []
            for i in range(count):
                at = jnp.minimum(offset_ref[2 * pair + sub, experts[i]] + w * window, totals[i])
                ys.append(y_refs[i][pl.ds(at, window)].reshape(window * GRAN, width))
            return jnp.dot(hot, jnp.concatenate(ys, axis=0), preferred_element_type=F32)

        def scaled(sub, back, r):
            return back[r * LANES : (r + 1) * LANES] * gate_cols[:, sub * BLOCK_ROWS + r : sub * BLOCK_ROWS + r + 1]

        @pl.when(pair >= 2)
        def _():
            out_copy(pair, slot).wait()

        for sub in range(2):
            b = 2 * pair + sub
            hot = hot_ref[pl.ds(pl.multiple_of(b * block_tok, block_tok), block_tok), :]
            back = window_rows(sub, 0, hot)
            for r in range(BLOCK_ROWS):
                source = pl.ds(pl.multiple_of(b * block_tok + r * LANES, LANES), LANES)
                at = slice((sub * BLOCK_ROWS + r) * LANES, (sub * BLOCK_ROWS + r + 1) * LANES)
                o_buf[slot, at, :] = (part_ref[source, :].astype(F32) + scaled(sub, back, r)).astype(BF16)

        for sub in range(2):
            b = 2 * pair + sub
            longest = count_ref[b, experts[0]]
            for e in experts[1:]:
                longest = jnp.maximum(longest, count_ref[b, e])

            def more(w, _):
                local = local_slots(experts, pos_ref[rows8, :], ids_ref[rows8, :], [start_ref[b, e] + w * window for e in experts])
                back = window_rows(sub, w, hot_rows(local, window, sub))
                for r in range(BLOCK_ROWS):
                    at = slice((sub * BLOCK_ROWS + r) * LANES, (sub * BLOCK_ROWS + r + 1) * LANES)
                    o_buf[slot, at, :] = (o_buf[slot, at, :].astype(F32) + scaled(sub, back, r)).astype(BF16)
                return 0

            lax.fori_loop(1, (longest + window - 1) // window, more, 0)
        out_copy(pair, slot).start()
        return 0

    lax.fori_loop(0, blocks // 2, per_pair, 0)
    for slot in range(2):
        out_copy(0, slot).wait()


def local_slots(experts, pos8, ids8, firsts):
    local = []
    for e, first in zip(experts, firsts):
        mine = (ids8 == e) & (pos8 >= 0)
        local.append(jnp.transpose(jnp.where(mine, pos8 - first * GRAN, -1).astype(F32)))
    return local


def hot_rows(local, window, sub):
    lane = iota((LANES, window * GRAN), 1).astype(F32)
    hot = []
    for r in range(sub * BLOCK_ROWS, (sub + 1) * BLOCK_ROWS):
        hot.append(jnp.concatenate([(lane == cols[:, r : r + 1]).astype(F32).astype(BF16) for cols in local], axis=1))
    return jnp.concatenate(hot, axis=0)


def combine_kernel(slots, bits, window, start_ref, ys_ref, pos_ref, gate_ref, ids_ref, out_ref, hot_ref):
    experts = expert_names(bits)
    rows = pos_ref.shape[0]
    pos_cols = jnp.transpose(pos_ref[...].astype(F32))
    later = (ids_ref[...] == experts[0]) | (ids_ref[...] == experts[1])
    gate_cols = jnp.transpose(jnp.where(later, 0.0, gate_ref[...]))
    grans = slots // GRAN
    upper = iota(pos_ref.shape, 0) < BLOCK_ROWS
    pair = pl.program_id(0)
    firsts = [jnp.where(upper, start_ref[2 * pair, e], start_ref[2 * pair + 1, e]) for e in experts]
    local = local_slots(experts, pos_ref[...], ids_ref[...], firsts)
    slot_iota = iota((LANES, slots), 1).astype(F32)
    for sub in range(rows // BLOCK_ROWS):
        row0 = sub * BLOCK_ROWS
        y = ys_ref[pl.ds((pl.program_id(0) * (rows // BLOCK_ROWS) + sub) * grans, grans)].reshape(slots, ys_ref.shape[2])
        hot = [(slot_iota == pos_cols[:, r : r + 1]).astype(F32).astype(BF16) for r in range(row0, row0 + BLOCK_ROWS)]
        back = jnp.dot(jnp.concatenate(hot, axis=0), y, preferred_element_type=F32)
        for r in range(BLOCK_ROWS):
            at = pl.ds(pl.multiple_of(((pl.program_id(0) * rows) + row0 + r) * LANES, LANES), LANES)
            scaled = back[r * LANES : (r + 1) * LANES] * gate_cols[:, row0 + r : row0 + r + 1]
            out_ref[at, :] = scaled.astype(BF16)
        block = pl.ds(pl.multiple_of((2 * pair + sub) * BLOCK_ROWS * LANES, BLOCK_ROWS * LANES), BLOCK_ROWS * LANES)
        hot_ref[block, :] = hot_rows(local, window, sub)


def vmem():
    return pl.BlockSpec(memory_space=pltpu.VMEM)


def smem():
    return pl.BlockSpec(memory_space=pltpu.SMEM)


def hbm():
    return pl.BlockSpec(memory_space=pl.ANY)


def solution(mesh):
    num_experts = mesh.shape["ep_b"] * mesh.shape["ep_a"]
    tok_spec = P(("dp",) + EXPERT_AXES)
    expert_spec = P(EXPERT_AXES)

    def swap(value, bit):
        return lax.ppermute(value, EXPERT_AXES, [(e, e ^ bit) for e in range(num_experts)])

    def inner_step(tokens, expert_ids, route_order, w_route, expert_keys, value_a11, w_in, b_in, w_out, b_out):
        tok_dev, width = tokens.shape[1], tokens.shape[2]
        hidden = w_in.shape[2]
        router = w_route.shape[1]
        capacity = (5 * tok_dev + 4 * num_experts - 1) // (4 * num_experts)
        rows = tok_dev // LANES
        blocks = rows // BLOCK_ROWS
        slots = -(-(BLOCK_ROWS * LANES + num_experts * (GRAN - 1)) // LANES) * LANES
        span = slots // GRAN

        first, second = w_in[0], w_out[0]
        x_first, y_first = swap(first, 2), swap(first, 4)
        x_second, y_second = swap(second, 2), swap(second, 4)
        c_first, c_second = swap(first, 1), swap(second, 1)
        own_bias = jnp.concatenate([b_in, b_out], axis=1)
        bias = [own_bias] + [swap(own_bias, bit) for bit in range(1, num_experts)]

        ids, order = expert_ids.reshape(rows, LANES), route_order.reshape(rows, LANES)
        unit = 2 * BLOCK_ROWS
        small = functools.partial(pl.BlockSpec, index_map=lambda i: (0, 0))
        whole = small((rows, LANES))
        table = small((blocks, LANES))
        xs_shape = (blocks * span + 8, GRAN, width)
        pos, starts, counts, offsets, lists, gate, xs = pl.pallas_call(
            functools.partial(dispatch_kernel, router, num_experts, capacity, slots),
            out_shape=(
                jax.ShapeDtypeStruct((rows, LANES), jnp.int32),
                jax.ShapeDtypeStruct((blocks, LANES), jnp.int32),
                jax.ShapeDtypeStruct((blocks, LANES), jnp.int32),
                jax.ShapeDtypeStruct((blocks, LANES), jnp.int32),
                jax.ShapeDtypeStruct((num_experts, LANES), jnp.int32),
                jax.ShapeDtypeStruct((rows, LANES), F32),
                pltpu.VMEM(xs_shape, BF16),
            ),
            grid=(rows // unit,),
            in_specs=[
                smem(),
                whole,
                whole,
                small((width, router)),
                small((num_experts, router)),
                pl.BlockSpec((unit * LANES, width), lambda i: (i, 0)),
            ],
            out_specs=(
                whole,
                table,
                table,
                table,
                small((num_experts, LANES)),
                pl.BlockSpec((unit, LANES), lambda i: (i, 0)),
                vmem(),
            ),
            scratch_shapes=[pltpu.VMEM((router + 4 * num_experts, width), BF16)],
            cost_estimate=pl.CostEstimate(flops=9 * 10**9, bytes_accessed=14 * 10**6, transcendentals=0),
            compiler_params=pltpu.CompilerParams(vmem_limit_bytes=12 * 2**20),
            name="dispatch",
        )(value_a11.reshape(1, 1), *[pltpu.with_memory_space_constraint(array, pltpu.HBM) for array in (ids, order, w_route, expert_keys, tokens[0])])

        most = -(-(capacity + blocks * (GRAN - 1)) // (32 * GRAN)) * 32
        tile, window = 32, 8
        held = lambda array: pltpu.with_memory_space_constraint(array, pltpu.VMEM)

        spare = blocks * span
        limit = pltpu.CompilerParams(vmem_limit_bytes=8 * 2**20)
        tables = (counts, offsets, lists)

        def cost(flops):
            return pl.CostEstimate(flops=flops, bytes_accessed=10**6, transcendentals=0)

        def up(bits, xs, firsts):
            n = len(bits)
            pieces = len(firsts[0])
            return pl.pallas_call(
                functools.partial(up_kernel, bits, pieces, tile, most),
                out_shape=pltpu.VMEM((n * most * GRAN, hidden), BF16),
                in_specs=[smem()] * 3 + [vmem()] * (1 + n * pieces + n),
                out_specs=vmem(),
                cost_estimate=cost(2 * n * 10**9),
                compiler_params=limit,
            )(*tables, held(xs), *[held(piece) for expert in firsts for piece in expert], *[bias[bit] for bit in bits])

        def down(bits, place, xs, h, seconds):
            return pl.pallas_call(
                functools.partial(down_kernel, bits, place, tile, most, spare),
                out_shape=pltpu.VMEM(xs.shape, BF16),
                in_specs=[smem()] * 3 + [vmem()] * (2 + 2 * len(bits)),
                out_specs=vmem(),
                input_output_aliases={3: 0},
                cost_estimate=cost(2 * len(bits) * 10**9),
                compiler_params=limit,
            )(*tables, held(xs), held(h), *map(held, seconds), *[bias[bit] for bit in bits])

        xs = pl.pallas_call(
            functools.partial(expert_kernel, (0, 1), tile, spare),
            out_shape=pltpu.VMEM(xs.shape, BF16),
            in_specs=[smem()] * 3 + [vmem()] * 7,
            out_specs=vmem(),
            scratch_shapes=[pltpu.VMEM((tile * GRAN, hidden), BF16)],
            input_output_aliases={3: 0},
            cost_estimate=cost(6 * 10**9),
            compiler_params=limit,
            name="experts0",
        )(*tables, held(xs), held(first), held(c_first), held(second), held(c_second), bias[0], bias[1])

        x_first, y_first, xs = lax.optimization_barrier((x_first, y_first, xs))
        cut = width - LANES
        d_top, d_low = swap(x_first[:cut], 4), swap(y_first[cut:], 2)
        cx_first, cy_first = swap(x_first, 1), swap(y_first, 1)
        h = up((2, 4, 3, 5), xs, ((x_first,), (y_first,), (cx_first,), (cy_first,)))
        x_second, y_second, h = lax.optimization_barrier((x_second, y_second, h))
        edge = hidden // 3
        e_top, e_low = swap(x_second[:edge], 4), swap(y_second[edge:], 2)
        cx_second, cy_second = swap(x_second, 1), swap(y_second, 1)
        xs = down((2, 4), 0, xs, h, (x_second, y_second))
        xs = down((3, 5), 2, xs, h, (cx_second, cy_second))
        part, hot = pl.pallas_call(
            functools.partial(combine_kernel, slots, (6, 7), window),
            out_shape=(pltpu.VMEM((tok_dev, width), BF16), pltpu.VMEM((tok_dev, 2 * window * GRAN), BF16)),
            grid=(rows // unit,),
            in_specs=[
                smem(),
                vmem(),
                pl.BlockSpec((unit, LANES), lambda i: (i, 0)),
                pl.BlockSpec((unit, LANES), lambda i: (i, 0)),
                pl.BlockSpec((unit, LANES), lambda i: (i, 0)),
            ],
            out_specs=(vmem(), vmem()),
            cost_estimate=cost(5 * 10**9),
            compiler_params=limit,
            name="combine",
        )(starts, held(xs), pos, gate, ids)
        d_top, d_low, part, hot = lax.optimization_barrier((d_top, d_low, part, hot))
        firsts = ((d_top, d_low), (swap(d_top, 1), swap(d_low, 1)))
        h = up((6, 7), xs, firsts)
        e_top, e_low, h = lax.optimization_barrier((e_top, e_low, h))
        ce_top, ce_low = swap(e_top, 1), swap(e_low, 1)
        y = pl.pallas_call(
            functools.partial(half_kernel, (6, 7), tile, most, window),
            out_shape=pltpu.VMEM((most + window, GRAN, width), BF16),
            in_specs=[smem()] * 2 + [vmem()] * 4,
            out_specs=vmem(),
            cost_estimate=cost(2 * 10**9),
            compiler_params=limit,
            name="half",
        )(counts, offsets, held(h), held(e_top), held(e_low), bias[6])
        out = pl.pallas_call(
            functools.partial(final_kernel, (6, 7), tile, most, window),
            out_shape=jax.ShapeDtypeStruct((tok_dev, width), BF16),
            in_specs=[smem()] * 3 + [vmem()] * (7 + 3),
            out_specs=hbm(),
            scratch_shapes=[
                pltpu.VMEM((most + window, GRAN, width), BF16),
                pltpu.VMEM((2, 2 * BLOCK_ROWS * LANES, width), BF16),
                pltpu.SemaphoreType.DMA((2,)),
            ],
            cost_estimate=cost(5 * 10**9),
            compiler_params=limit,
            name="final",
        )(starts, counts, offsets, pos, gate, ids, held(hot), held(h), held(part), held(y), held(ce_top), held(ce_low), bias[7])
        return out[None]

    return jax.shard_map(
        inner_step,
        mesh=mesh,
        in_specs=(tok_spec, tok_spec, tok_spec, P(), P(), P(), expert_spec, expert_spec, expert_spec, expert_spec),
        out_specs=tok_spec,
        check_vma=False,
    )
```

```python
import functools

import jax
import jax.numpy as jnp
from jax import lax
from jax.experimental import pallas as pl
from jax.experimental.pallas import tpu as pltpu
from jax.sharding import PartitionSpec as P


EXPERT_AXES = ("ep_b", "ep_a")

LANES = 128
BLOCK_ROWS = 4
GRAN = 16
LIMIT = 5
BF16 = jnp.bfloat16
F32 = jnp.float32
NT = (((1,), (1,)), ((), ()))


def iota(shape, dim):
    return lax.broadcasted_iota(jnp.int32, shape, dim)


def plan_step(num_experts, capacity, span, ids_ref, ord_ref, wr_ref, keys_ref, pos_ref, start_ref, count_ref, offset_ref, list_ref, wt_ref):
    rows = ids_ref.shape[0]
    blocks = rows // BLOCK_ROWS
    place = jnp.zeros((2 * rows, LANES), F32)
    hi_iota = iota((rows, LANES), 0)
    lo_iota = iota((LANES, LANES), 0)
    lane_val = iota((rows, LANES), 1).astype(F32)
    for chunk in range(rows // 8):
        left, right = [], []
        for r in range(8 * chunk, 8 * chunk + 8):
            order_row = ord_ref[r : r + 1, :]
            hit = hi_iota == (order_row >> 7)
            upper = jnp.where(hit, F32(r), 0.0).astype(BF16)
            lower = jnp.where(hit, lane_val, 0.0).astype(BF16)
            left.append(jnp.concatenate([upper, lower], axis=0))
            right.append(jnp.where(lo_iota == (order_row & 127), 1.0, 0.0).astype(BF16))
        place += lax.dot_general(jnp.concatenate(left, axis=1), jnp.concatenate(right, axis=1), NT, preferred_element_type=F32)
    place = (place[:rows] * LANES + place[rows:]).astype(jnp.int32)
    ids = ids_ref[...]
    mask = (ids[None] == iota((num_experts, rows, LANES), 0)).astype(F32)

    def narrow(step, bound):
        trial = bound + (2 * rows * LANES >> (step + 1))
        admitted = jnp.where(place[None] < trial, mask, 0.0)
        total = jnp.sum(jnp.sum(admitted, axis=1, keepdims=True), axis=2, keepdims=True)
        return jnp.where(total <= capacity, trial, bound)

    steps = (rows * LANES).bit_length()
    bound = lax.fori_loop(0, steps, narrow, jnp.zeros((num_experts, 1, 1), jnp.int32))
    kept = jnp.where(place[None] < bound, mask, 0.0)
    kept2 = kept.reshape(num_experts * rows, LANES).astype(BF16)
    before = (iota((LANES, LANES), 0) < iota((LANES, LANES), 1)).astype(BF16)
    lane_prefix = jnp.dot(kept2, before, preferred_element_type=F32)
    row_total = jnp.dot(kept2, jnp.ones((LANES, LANES), BF16), preferred_element_type=F32).astype(BF16)
    row_a, row_b = iota((rows, rows), 0), iota((rows, rows), 1)
    same = row_a // BLOCK_ROWS == row_b // BLOCK_ROWS
    earlier = (same & (row_b < row_a)).astype(BF16)
    same = same.astype(BF16)
    pick = (iota((blocks, rows), 1) == iota((blocks, rows), 0) * BLOCK_ROWS).astype(BF16)
    lane = iota((blocks, LANES), 1)
    slot = jnp.full((rows, LANES), -1, jnp.int32)
    first = jnp.zeros((rows, LANES), jnp.int32)
    starts = jnp.zeros((blocks, LANES), F32)
    counts = jnp.zeros((blocks, LANES), F32)
    offsets = jnp.zeros((blocks, LANES), F32)
    block_iota = iota((blocks, LANES), 0)
    past = (iota((blocks, blocks), 1) < iota((blocks, blocks), 0)).astype(BF16)
    for e in range(num_experts):
        part = slice(e * rows, (e + 1) * rows)
        row_prefix = jnp.dot(earlier, row_total[part], preferred_element_type=F32)
        in_block = jnp.dot(same, row_total[part], preferred_element_type=F32).astype(jnp.int32)
        grans = (in_block + (GRAN - 1)) >> 4
        here = first * GRAN + (row_prefix + lane_prefix[part]).astype(jnp.int32)
        slot = jnp.where(kept[e] > 0.0, here, slot)
        first_b = jnp.dot(pick, first.astype(F32).astype(BF16), preferred_element_type=F32)
        count_b = jnp.dot(pick, grans.astype(F32).astype(BF16), preferred_element_type=F32)
        offset_b = jnp.dot(past, count_b.astype(BF16), preferred_element_type=F32)
        starts += jnp.where(lane == e, first_b, 0.0)
        counts += jnp.where(lane == e, count_b, 0.0)
        offsets += jnp.where(lane == e, offset_b, 0.0)
        index = (lane - offset_b.astype(jnp.int32) + first_b.astype(jnp.int32) + block_iota * span).astype(F32)
        inside = (lane.astype(F32) >= offset_b) & (lane.astype(F32) < offset_b + count_b)
        index = jnp.sum(jnp.where(inside, index - blocks * span, 0.0), axis=0, keepdims=True)
        list_ref[e : e + 1, :] = index.astype(jnp.int32) + blocks * span
        first = first + grans
    pos_ref[...] = slot
    start_ref[...] = starts.astype(jnp.int32)
    offset_ref[...] = offsets.astype(jnp.int32)
    count_ref[...] = counts.astype(jnp.int32)
    wr = wr_ref[...]
    router = wr.shape[1]
    eye = (iota((router, router), 0) == iota((router, router), 1)).astype(BF16)
    keys = keys_ref[...].astype(F32)
    unit = keys / jnp.sqrt(jnp.sum(keys * keys, axis=1, keepdims=True))
    folded = lax.dot_general(unit, wr.astype(F32), NT, preferred_element_type=F32, precision=lax.Precision.HIGHEST)
    part_a = folded.astype(BF16)
    rest = folded - part_a.astype(F32)
    part_b = rest.astype(BF16)
    part_c = (rest - part_b.astype(F32)).astype(BF16)
    wt_ref[0:router, :] = lax.dot_general(eye, wr, NT, preferred_element_type=F32).astype(BF16)
    tail = jnp.concatenate([part_a.astype(F32), part_b.astype(F32), part_c.astype(F32), jnp.zeros_like(folded)], axis=0)
    wt_ref[router:, :] = tail.astype(BF16)


def over_lanes(rows):
    cols = [jnp.transpose(jnp.broadcast_to(rows[r : r + 1], (LANES, LANES))) for r in range(rows.shape[0])]
    return jnp.concatenate(cols, axis=0)


def dispatch_kernel(
    router, num_experts, capacity, slots, tau_ref, ids_ref, ord_ref, wr_ref, keys_ref, x_ref,
    start_ref, count_ref, offset_ref, list_ref, pos_ref, gate_ref, xs_ref, wt_ref,
):
    grans = slots // GRAN
    spare = start_ref.shape[0] * grans

    @pl.when(pl.program_id(0) == 0)
    def _():
        plan_step(
            num_experts, capacity, grans, ids_ref, ord_ref, wr_ref, keys_ref,
            pos_ref, start_ref, count_ref, offset_ref, list_ref, wt_ref,
        )
        xs_ref[spare:] = jnp.zeros((xs_ref.shape[0] - spare,) + xs_ref.shape[1:], BF16)

    rows = x_ref.shape[0] // LANES
    part = pl.ds(pl.multiple_of(pl.program_id(0) * rows, rows), rows)
    ids, pos = ids_ref[part, :], pos_ref[part, :]
    tau = tau_ref[0, 0]
    for sub in range(rows // BLOCK_ROWS):
        row0 = sub * BLOCK_ROWS
        x = x_ref[row0 * LANES : (row0 + BLOCK_ROWS) * LANES, :]
        proj = lax.dot_general(wt_ref[...], x, NT, preferred_element_type=F32)
        square = jnp.sum(proj[:router] * proj[:router], axis=0, keepdims=True)
        ne = num_experts
        logits = proj[router : router + ne] + proj[router + ne : router + 2 * ne] + proj[router + 2 * ne : router + 3 * ne]
        logits = logits / jnp.sqrt(square) / tau
        expo = jnp.exp(logits - jnp.max(logits, axis=0, keepdims=True))
        prob = expo / jnp.sum(expo, axis=0, keepdims=True)
        id_row = jnp.concatenate([ids[r : r + 1] for r in range(row0, row0 + BLOCK_ROWS)], axis=1)
        gate = jnp.sum(jnp.where(iota(prob.shape, 0) == id_row, prob, 0.0), axis=0, keepdims=True)
        for r in range(BLOCK_ROWS):
            gate_ref[row0 + r : row0 + r + 1, :] = gate[:, r * LANES : (r + 1) * LANES]
        slot_iota = iota((slots, LANES), 0)
        hot = [(slot_iota == pos[r : r + 1]).astype(F32).astype(BF16) for r in range(row0, row0 + BLOCK_ROWS)]
        picked = jnp.dot(jnp.concatenate(hot, axis=1), x, preferred_element_type=F32).astype(BF16)
        at = pl.ds((pl.program_id(0) * (rows // BLOCK_ROWS) + sub) * grans, grans)
        xs_ref[at] = picked.reshape(grans, GRAN, picked.shape[1])


def expert_names(bits):
    me = lax.axis_index("ep_b") * lax.axis_size("ep_a") + lax.axis_index("ep_a")
    return [me ^ bit for bit in bits]


def stacked_dot(left, refs, columns):
    total, at = None, 0
    for ref in refs:
        depth = ref.shape[0]
        part = jnp.dot(left[:, at : at + depth], ref[:, columns], preferred_element_type=F32)
        total = part if total is None else total + part
        at += depth
    return total


def split_bias(ref, hidden):
    return ref[:, 0:hidden].astype(F32), ref[:, hidden:].astype(F32)


def up_tile(x, refs, b1, h_ref, at):
    hidden = refs[0].shape[1]
    step = 256
    for c in range(0, hidden, step):
        pre = stacked_dot(x, refs, slice(c, c + step)) + b1[:, c : c + step]
        act = 0.5 * pre * (1.0 + lax.erf(pre * F32(0.5**0.5)))
        h_ref[at, c : c + step] = act.astype(BF16)


def granules(e, count_ref, offset_ref):
    last = count_ref.shape[0] - 1
    return offset_ref[last, e] + count_ref[last, e]


def tile_names(e, t, tile, list_ref):
    return [list_ref[e, t * tile + k] for k in range(tile)]


def put_rows(names, spare, y, out_ref):
    for k, name in enumerate(names):
        out_ref[jnp.where(name == spare, spare + 15, name)] = y[k * GRAN : (k + 1) * GRAN]


def expert_kernel(bits, tile, spare, count_ref, offset_ref, list_ref, xs_ref, *refs):
    count = len(bits)
    w1_refs, w2_refs, b_refs = refs[:count], refs[count : 2 * count], refs[2 * count : 3 * count]
    out_ref, h_buf = refs[3 * count :]
    hidden = h_buf.shape[1]
    for i, e in enumerate(expert_names(bits)):
        b1, b2 = split_bias(b_refs[i], hidden)

        def per_tile(t, _):
            names = tile_names(e, t, tile, list_ref)
            up_tile(jnp.concatenate([xs_ref[name] for name in names], axis=0), [w1_refs[i]], b1, h_buf, slice(None))
            y = stacked_dot(h_buf[...], [w2_refs[i]], slice(None)) + b2
            put_rows(names, spare, y.astype(BF16), out_ref)
            return 0

        lax.fori_loop(0, (granules(e, count_ref, offset_ref) + tile - 1) // tile, per_tile, 0)


def up_kernel(bits, pieces, tile, most, count_ref, offset_ref, list_ref, xs_ref, *refs):
    count = len(bits)
    w1_refs = [refs[i * pieces : (i + 1) * pieces] for i in range(count)]
    b_refs = refs[count * pieces : count * pieces + count]
    h_ref = refs[count * pieces + count]
    hidden = h_ref.shape[1]
    for i, e in enumerate(expert_names(bits)):
        b1, _ = split_bias(b_refs[i], hidden)

        def per_tile(t, _):
            names = tile_names(e, t, tile, list_ref)
            at = pl.ds(pl.multiple_of((i * most + t * tile) * GRAN, tile * GRAN), tile * GRAN)
            up_tile(jnp.concatenate([xs_ref[name] for name in names], axis=0), w1_refs[i], b1, h_ref, at)
            return 0

        lax.fori_loop(0, (granules(e, count_ref, offset_ref) + tile - 1) // tile, per_tile, 0)


def down_kernel(bits, first, tile, most, spare, count_ref, offset_ref, list_ref, xs_ref, h_ref, *refs):
    count = len(bits)
    w2_refs, b_refs, out_ref = refs[:count], refs[count : 2 * count], refs[2 * count]
    del xs_ref
    for i, e in enumerate(expert_names(bits)):
        _, b2 = split_bias(b_refs[i], h_ref.shape[1])

        def per_tile(t, _):
            names = tile_names(e, t, tile, list_ref)
            at = pl.ds(pl.multiple_of(((first + i) * most + t * tile) * GRAN, tile * GRAN), tile * GRAN)
            y = stacked_dot(h_ref[at, :], [w2_refs[i]], slice(None)) + b2
            put_rows(names, spare, y.astype(BF16), out_ref)
            return 0

        lax.fori_loop(0, (granules(e, count_ref, offset_ref) + tile - 1) // tile, per_tile, 0)


def compact_down(total, tile, window, w2_refs, b_ref, h_ref, y_ref, after=lambda t, state: state):
    width = y_ref.shape[2]
    _, b2 = split_bias(b_ref, h_ref.shape[1])

    def per_tile(t, state):
        at = pl.ds(pl.multiple_of(t * tile * GRAN, tile * GRAN), tile * GRAN)
        y = stacked_dot(h_ref[at, :], w2_refs, slice(None)) + b2
        y_ref[pl.ds(t * tile, tile)] = y.astype(BF16).reshape(tile, GRAN, width)
        y_ref[pl.ds((t + 1) * tile, window)] = jnp.zeros((window, GRAN, width), BF16)
        return after(t, state)

    tiles = (total + tile - 1) // tile

    @pl.when(tiles == 0)
    def _():
        y_ref[pl.ds(0, window)] = jnp.zeros((window, GRAN, width), BF16)

    return lax.fori_loop(0, tiles, per_tile, jnp.int32(0))


def half_kernel(bits, tile, window, count_ref, offset_ref, h_ref, *refs):
    total = granules(expert_names(bits)[0], count_ref, offset_ref)
    compact_down(total, tile, window, refs[:-2], refs[-2], h_ref, refs[-1])


def final_kernel(bits, tile, window, start_ref, count_ref, offset_ref, slot_ref, gate_ref, h_ref, part_ref, y_ref, *refs):
    experts = expert_names(bits)
    out_ref, y_buf, o_buf, o_sem = refs[-4:]
    y_refs = (y_ref, y_buf)
    blocks = start_ref.shape[0]
    width = part_ref.shape[1]
    block_tok = BLOCK_ROWS * LANES
    totals = [granules(e, count_ref, offset_ref) for e in experts]

    def rows_of(i, w, b):
        at = jnp.minimum(offset_ref[b, experts[i]] + w * window, totals[i])
        return y_refs[i][pl.ds(at, window)].reshape(window * GRAN, width)

    def out_copy(pair, slot):
        rows = pl.ds(pl.multiple_of(pair * 2 * block_tok, 2 * block_tok), 2 * block_tok)
        return pltpu.make_async_copy(o_buf.at[slot], out_ref.at[rows], o_sem.at[slot])

    def add(b, w, sub, turn, slots, gates, base_ref, base_at):
        part = slice(sub * BLOCK_ROWS, (sub + 1) * BLOCK_ROWS)
        back = window_dot(experts, w, b, start_ref, count_ref, over_lanes(slots[part]), rows_of)
        gate = over_lanes(gates[part])
        for c in range(0, width, LANES):
            base = base_ref[base_at, c : c + LANES].astype(F32)
            o_buf[turn, sub * block_tok : (sub + 1) * block_tok, c : c + LANES] = (base + back[:, c : c + LANES] * gate).astype(BF16)

    def per_pair(pair, _):
        turn = pair % 2
        rows8 = pl.ds(pl.multiple_of(pair * 2 * BLOCK_ROWS, 2 * BLOCK_ROWS), 2 * BLOCK_ROWS)
        slots, gates = slot_ref[rows8, :].astype(F32), gate_ref[rows8, :]

        @pl.when(pair >= 2)
        def _():
            out_copy(pair, turn).wait()

        for sub in range(2):
            b = 2 * pair + sub
            add(b, 0, sub, turn, slots, gates, part_ref, pl.ds(pl.multiple_of(b * block_tok, block_tok), block_tok))
        for sub in range(2):
            b = 2 * pair + sub

            def more(w, _):
                add(b, w, sub, turn, slots, gates, o_buf.at[turn], slice(sub * block_tok, (sub + 1) * block_tok))
                return 0

            lax.fori_loop(1, (longest_run(experts, b, count_ref) + window - 1) // window, more, 0)
        out_copy(pair, turn).start()
        return 0

    def ready_pairs(t, done):
        ready = 0
        for pair in range(blocks // 2):
            end = offset_ref[2 * pair + 1, experts[-1]] + count_ref[2 * pair + 1, experts[-1]]
            ready = ready + jnp.where(end <= (t + 1) * tile, 1, 0)
        lax.fori_loop(done, ready, per_pair, 0)
        return ready

    done = compact_down(totals[-1], tile, window, refs[:-5], refs[-5], h_ref, y_buf, ready_pairs)
    lax.fori_loop(done, blocks // 2, per_pair, 0)
    for slot in range(2):
        out_copy(0, slot).wait()


def window_dot(experts, w, b, start_ref, count_ref, slot, rows_of):
    lane = iota((1, LANES), 1)
    hot = []
    for e in experts:
        index = lane + w * LANES
        name = jnp.where(index < count_ref[b, e] * GRAN, index + start_ref[b, e] * GRAN, -2)
        hot.append((slot == name.astype(F32)).astype(F32).astype(BF16))
    return jnp.dot(jnp.concatenate(hot, axis=1), jnp.concatenate([rows_of(e, w, b) for e in range(len(experts))], axis=0), preferred_element_type=F32)


def longest_run(experts, b, count_ref):
    longest = count_ref[b, experts[0]]
    for e in experts[1:]:
        longest = jnp.maximum(longest, count_ref[b, e])
    return longest


def part_kernel(bits, fresh, window, span, start_ref, count_ref, xs_ref, slot_ref, gate_ref, *refs):
    experts = expert_names(bits)
    out_ref = refs[-1]
    width = xs_ref.shape[2]
    block_tok = BLOCK_ROWS * LANES

    def rows_of(i, w, b):
        at = jnp.minimum(b * span + start_ref[b, experts[i]] + w * window, xs_ref.shape[0] - 1 - window)
        return xs_ref[pl.ds(at, window)].reshape(window * GRAN, width)

    def add(b, w, slot, gate, fresh):
        back = window_dot(experts, w, b, start_ref, count_ref, slot, rows_of)
        at = pl.ds(pl.multiple_of(b * block_tok, block_tok), block_tok)
        for c in range(0, width, LANES):
            scaled = back[:, c : c + LANES] * gate
            if not fresh:
                scaled = scaled + out_ref[at, c : c + LANES].astype(F32)
            out_ref[at, c : c + LANES] = scaled.astype(BF16)

    def per_group(group, _):
        row0 = pl.multiple_of(group * 4 * BLOCK_ROWS, 4 * BLOCK_ROWS)
        slots = slot_ref[pl.ds(row0, 4 * BLOCK_ROWS), :].astype(F32)
        gates = gate_ref[pl.ds(row0, 4 * BLOCK_ROWS), :]
        for sub in range(4):
            part = slice(sub * BLOCK_ROWS, (sub + 1) * BLOCK_ROWS)
            add(4 * group + sub, 0, over_lanes(slots[part]), over_lanes(gates[part]), fresh)
        for sub in range(4):
            part = slice(sub * BLOCK_ROWS, (sub + 1) * BLOCK_ROWS)

            def more(w, _):
                add(4 * group + sub, w, over_lanes(slots[part]), over_lanes(gates[part]), False)
                return 0

            lax.fori_loop(1, (longest_run(experts, 4 * group + sub, count_ref) + window - 1) // window, more, 0)
        return 0

    lax.fori_loop(0, start_ref.shape[0] // 4, per_group, 0)


def vmem():
    return pl.BlockSpec(memory_space=pltpu.VMEM)


def smem():
    return pl.BlockSpec(memory_space=pltpu.SMEM)


def hbm():
    return pl.BlockSpec(memory_space=pl.ANY)


def solution(mesh):
    num_experts = mesh.shape["ep_b"] * mesh.shape["ep_a"]
    tok_spec = P(("dp",) + EXPERT_AXES)
    expert_spec = P(EXPERT_AXES)

    def swap(value, bit):
        return lax.ppermute(value, EXPERT_AXES, [(e, e ^ bit) for e in range(num_experts)])

    def inner_step(tokens, expert_ids, route_order, w_route, expert_keys, value_a11, w_in, b_in, w_out, b_out):
        tok_dev, width = tokens.shape[1], tokens.shape[2]
        hidden = w_in.shape[2]
        router = w_route.shape[1]
        capacity = (5 * tok_dev + 4 * num_experts - 1) // (4 * num_experts)
        rows = tok_dev // LANES
        blocks = rows // BLOCK_ROWS
        slots = -(-(BLOCK_ROWS * LANES + num_experts * (GRAN - 1)) // LANES) * LANES
        span = slots // GRAN

        first, second = w_in[0], w_out[0]
        x_first, y_first = swap(first, 2), swap(first, 4)
        x_second, y_second = swap(second, 2), swap(second, 4)
        c_first, c_second = swap(first, 1), swap(second, 1)
        own_bias = jnp.concatenate([b_in, b_out], axis=1)
        bias = [own_bias] + [swap(own_bias, bit) for bit in range(1, num_experts)]

        ids, order = expert_ids.reshape(rows, LANES), route_order.reshape(rows, LANES)
        unit = 2 * BLOCK_ROWS
        small = functools.partial(pl.BlockSpec, index_map=lambda i: (0, 0))
        whole = small((rows, LANES))
        table = small((blocks, LANES))
        xs_shape = (blocks * span + 16, GRAN, width)
        starts, counts, offsets, lists, slot, gate, xs = pl.pallas_call(
            functools.partial(dispatch_kernel, router, num_experts, capacity, slots),
            out_shape=(
                jax.ShapeDtypeStruct((blocks, LANES), jnp.int32),
                jax.ShapeDtypeStruct((blocks, LANES), jnp.int32),
                jax.ShapeDtypeStruct((blocks, LANES), jnp.int32),
                jax.ShapeDtypeStruct((num_experts, LANES), jnp.int32),
                jax.ShapeDtypeStruct((rows, LANES), jnp.int32),
                jax.ShapeDtypeStruct((rows, LANES), F32),
                pltpu.VMEM(xs_shape, BF16),
            ),
            grid=(rows // unit,),
            in_specs=[
                smem(),
                whole,
                whole,
                small((width, router)),
                small((num_experts, router)),
                pl.BlockSpec((unit * LANES, width), lambda i: (i, 0)),
            ],
            out_specs=(
                table, table, table, small((num_experts, LANES)),
                whole, pl.BlockSpec((unit, LANES), lambda i: (i, 0)), vmem(),
            ),
            scratch_shapes=[pltpu.VMEM((router + 4 * num_experts, width), BF16)],
            cost_estimate=pl.CostEstimate(flops=9 * 10**9, bytes_accessed=14 * 10**6, transcendentals=0),
            compiler_params=pltpu.CompilerParams(vmem_limit_bytes=12 * 2**20),
            name="dispatch",
        )(value_a11.reshape(1, 1), *[pltpu.with_memory_space_constraint(array, pltpu.HBM) for array in (ids, order, w_route, expert_keys, tokens[0])])

        most = -(-(capacity + blocks * (GRAN - 1)) // (32 * GRAN)) * 32
        tile, window = 32, 8
        held = lambda array: pltpu.with_memory_space_constraint(array, pltpu.VMEM)

        spare = blocks * span
        limit = pltpu.CompilerParams(vmem_limit_bytes=LIMIT * 2**20)
        tables = (counts, offsets, lists)

        def cost(flops):
            return pl.CostEstimate(flops=flops, bytes_accessed=10**6, transcendentals=0)

        def up(bits, xs, firsts):
            n = len(bits)
            pieces = len(firsts[0])
            return pl.pallas_call(
                functools.partial(up_kernel, bits, pieces, tile, most),
                out_shape=pltpu.VMEM((n * most * GRAN, hidden), BF16),
                in_specs=[smem()] * 3 + [vmem()] * (1 + n * pieces + n),
                out_specs=vmem(),
                cost_estimate=cost(2 * n * 10**9),
                compiler_params=limit,
            )(*tables, held(xs), *[held(piece) for expert in firsts for piece in expert], *[bias[bit] for bit in bits])

        def down(bits, place, xs, h, seconds):
            return pl.pallas_call(
                functools.partial(down_kernel, bits, place, tile, most, spare),
                out_shape=pltpu.VMEM(xs.shape, BF16),
                in_specs=[smem()] * 3 + [vmem()] * (2 + 2 * len(bits)),
                out_specs=vmem(),
                input_output_aliases={3: 0},
                cost_estimate=cost(2 * len(bits) * 10**9),
                compiler_params=limit,
            )(*tables, held(xs), held(h), *map(held, seconds), *[bias[bit] for bit in bits])

        def partial(bits, xs, part):
            held_part = [] if part is None else [held(part)]
            return pl.pallas_call(
                functools.partial(part_kernel, bits, part is None, window, span),
                out_shape=pltpu.VMEM((tok_dev, width), BF16),
                in_specs=[smem()] * 2 + [vmem()] * (3 + len(held_part)),
                out_specs=vmem(),
                input_output_aliases={} if part is None else {5: 0},
                cost_estimate=cost(2 * len(bits) * 10**9),
                compiler_params=limit,
            )(starts, counts, held(xs), slot, gate, *held_part)

        x_first, y_first, xs = lax.optimization_barrier((x_first, y_first, xs))
        cut = width - LANES
        d_top, d_low = swap(x_first[:cut], 4), swap(y_first[cut:], 2)
        cx_first, cy_first = swap(x_first, 1), swap(y_first, 1)
        xs = pl.pallas_call(
            functools.partial(expert_kernel, (0, 1), tile, spare),
            out_shape=pltpu.VMEM(xs.shape, BF16),
            in_specs=[smem()] * 3 + [vmem()] * 7,
            out_specs=vmem(),
            scratch_shapes=[pltpu.VMEM((tile * GRAN, hidden), BF16)],
            input_output_aliases={3: 0},
            cost_estimate=cost(6 * 10**9),
            compiler_params=limit,
            name="experts0",
        )(*tables, held(xs), held(first), held(c_first), held(second), held(c_second), bias[0], bias[1])
        h = up((2, 4, 3, 5), xs, ((x_first,), (y_first,), (cx_first,), (cy_first,)))
        part = partial((0, 1), xs, None)
        x_second, y_second, h, part = lax.optimization_barrier((x_second, y_second, h, part))
        edge = hidden // 3
        e_top, e_low = swap(x_second[:edge], 4), swap(y_second[edge:], 2)
        cx_second, cy_second = swap(x_second, 1), swap(y_second, 1)
        xs = down((2, 4), 0, xs, h, (x_second, y_second))
        xs = down((3, 5), 2, xs, h, (cx_second, cy_second))
        part = partial((2, 4, 3, 5), xs, part)
        d_top, d_low, part = lax.optimization_barrier((d_top, d_low, part))
        cd_top, cd_low = swap(d_top, 1), swap(d_low, 1)
        h6 = up((6,), xs, ((d_top, d_low),))
        h6, cd_top, cd_low = lax.optimization_barrier((h6, cd_top, cd_low))
        h7 = up((7,), xs, ((cd_top, cd_low),))
        e_top, e_low, h6, h7 = lax.optimization_barrier((e_top, e_low, h6, h7))
        ce_top, ce_low = swap(e_top, 1), swap(e_low, 1)
        y = pl.pallas_call(
            functools.partial(half_kernel, (6,), tile, window),
            out_shape=pltpu.VMEM((most + window, GRAN, width), BF16),
            in_specs=[smem()] * 2 + [vmem()] * 4,
            out_specs=vmem(),
            cost_estimate=cost(2 * 10**9),
            compiler_params=limit,
            name="half",
        )(counts, offsets, held(h6), held(e_top), held(e_low), bias[6])
        out = pl.pallas_call(
            functools.partial(final_kernel, (6, 7), tile, window),
            out_shape=jax.ShapeDtypeStruct((tok_dev, width), BF16),
            in_specs=[smem()] * 3 + [vmem()] * (5 + 3),
            out_specs=hbm(),
            scratch_shapes=[
                pltpu.VMEM((most + window, GRAN, width), BF16),
                pltpu.VMEM((2, 2 * BLOCK_ROWS * LANES, width), BF16),
                pltpu.SemaphoreType.DMA((2,)),
            ],
            cost_estimate=cost(5 * 10**9),
            compiler_params=pltpu.CompilerParams(vmem_limit_bytes=7 * 2**20),
            name="final",
        )(starts, counts, offsets, slot, gate, held(h7), held(part), held(y), held(ce_top), held(ce_low), bias[7])
        return out[None]

    return jax.shard_map(
        inner_step,
        mesh=mesh,
        in_specs=(tok_spec, tok_spec, tok_spec, P(), P(), P(), expert_spec, expert_spec, expert_spec, expert_spec),
        out_specs=tok_spec,
        check_vma=False,
    )
```

```python
import functools

import jax
import jax.numpy as jnp
from jax import lax
from jax.experimental import pallas as pl
from jax.experimental.pallas import tpu as pltpu
from jax.sharding import PartitionSpec as P


EXPERT_AXES = ("ep_b", "ep_a")

LANES = 128
BLOCK_ROWS = 4
GRAN = 16
EXTRA = 8
TILE = 30
LIMIT = 5
BF16 = jnp.bfloat16
F32 = jnp.float32
NT = (((1,), (1,)), ((), ()))


def iota(shape, dim):
    return lax.broadcasted_iota(jnp.int32, shape, dim)


def plan_step(num_experts, capacity, span, ids_ref, ord_ref, wr_ref, keys_ref, pos_ref, start_ref, count_ref, offset_ref, list_ref, wt_ref):
    rows = ids_ref.shape[0]
    blocks = rows // BLOCK_ROWS
    place = jnp.zeros((2 * rows, LANES), F32)
    hi_iota = iota((rows, LANES), 0)
    lo_iota = iota((LANES, LANES), 0)
    lane_val = iota((rows, LANES), 1).astype(F32)
    for chunk in range(rows // 8):
        left, right = [], []
        for r in range(8 * chunk, 8 * chunk + 8):
            order_row = ord_ref[r : r + 1, :]
            hit = hi_iota == (order_row >> 7)
            upper = jnp.where(hit, F32(r), 0.0).astype(BF16)
            lower = jnp.where(hit, lane_val, 0.0).astype(BF16)
            left.append(jnp.concatenate([upper, lower], axis=0))
            right.append(jnp.where(lo_iota == (order_row & 127), 1.0, 0.0).astype(BF16))
        place += lax.dot_general(jnp.concatenate(left, axis=1), jnp.concatenate(right, axis=1), NT, preferred_element_type=F32)
    place = (place[:rows] * LANES + place[rows:]).astype(jnp.int32)
    ids = ids_ref[...]
    mask = (ids[None] == iota((num_experts, rows, LANES), 0)).astype(F32)

    steps = ((rows * LANES).bit_length() + 1) // 2

    def narrow(step, bound):
        unit = 4 ** (steps - 1) >> (2 * step)
        passed = jnp.zeros_like(bound)
        for k in range(1, 4):
            admitted = jnp.where(place[None] < bound + k * unit, mask, 0.0)
            total = jnp.sum(jnp.sum(admitted, axis=1, keepdims=True), axis=2, keepdims=True)
            passed = passed + jnp.where(total <= capacity, 1, 0)
        return bound + passed * unit

    bound = lax.fori_loop(0, steps, narrow, jnp.zeros((num_experts, 1, 1), jnp.int32))
    kept = jnp.where(place[None] < bound, mask, 0.0)
    kept2 = kept.reshape(num_experts * rows, LANES).astype(BF16)
    before = (iota((LANES, LANES), 0) < iota((LANES, LANES), 1)).astype(BF16)
    lane_prefix = jnp.dot(kept2, before, preferred_element_type=F32)
    row_total = jnp.dot(kept2, jnp.ones((LANES, LANES), BF16), preferred_element_type=F32).astype(BF16)
    row_a, row_b = iota((rows, rows), 0), iota((rows, rows), 1)
    same = row_a // BLOCK_ROWS == row_b // BLOCK_ROWS
    earlier = (same & (row_b < row_a)).astype(BF16)
    same = same.astype(BF16)
    pick = (iota((blocks, rows), 1) == iota((blocks, rows), 0) * BLOCK_ROWS).astype(BF16)
    lane = iota((blocks, LANES), 1)
    slot = jnp.full((rows, LANES), -1, jnp.int32)
    first = jnp.zeros((rows, LANES), jnp.int32)
    starts = jnp.zeros((blocks, LANES), F32)
    counts = jnp.zeros((blocks, LANES), F32)
    offsets = jnp.zeros((blocks, LANES), F32)
    block_iota = iota((blocks, LANES), 0)
    past = (iota((blocks, blocks), 1) < iota((blocks, blocks), 0)).astype(BF16)
    for e in range(num_experts):
        part = slice(e * rows, (e + 1) * rows)
        row_prefix = jnp.dot(earlier, row_total[part], preferred_element_type=F32)
        in_block = jnp.dot(same, row_total[part], preferred_element_type=F32).astype(jnp.int32)
        grans = (in_block + (GRAN - 1)) >> 4
        here = first * GRAN + (row_prefix + lane_prefix[part]).astype(jnp.int32)
        slot = jnp.where(kept[e] > 0.0, here, slot)
        first_b = jnp.dot(pick, first.astype(F32).astype(BF16), preferred_element_type=F32)
        count_b = jnp.dot(pick, grans.astype(F32).astype(BF16), preferred_element_type=F32)
        offset_b = jnp.dot(past, count_b.astype(BF16), preferred_element_type=F32)
        starts += jnp.where(lane == e, first_b, 0.0)
        counts += jnp.where(lane == e, count_b, 0.0)
        offsets += jnp.where(lane == e, offset_b, 0.0)
        index = (lane - offset_b.astype(jnp.int32) + first_b.astype(jnp.int32) + block_iota * span).astype(F32)
        inside = (lane.astype(F32) >= offset_b) & (lane.astype(F32) < offset_b + count_b)
        index = jnp.sum(jnp.where(inside, index - blocks * span, 0.0), axis=0, keepdims=True)
        list_ref[e : e + 1, :] = index.astype(jnp.int32) + blocks * span
        first = first + grans
    pos_ref[...] = slot
    start_ref[...] = starts.astype(jnp.int32)
    offset_ref[...] = offsets.astype(jnp.int32)
    count_ref[...] = counts.astype(jnp.int32)
    wr = wr_ref[...]
    router = wr.shape[1]
    eye = (iota((router, router), 0) == iota((router, router), 1)).astype(BF16)
    keys = keys_ref[...].astype(F32)
    unit = keys / jnp.sqrt(jnp.sum(keys * keys, axis=1, keepdims=True))
    folded = lax.dot_general(unit, wr.astype(F32), NT, preferred_element_type=F32, precision=lax.Precision.HIGHEST)
    part_a = folded.astype(BF16)
    rest = folded - part_a.astype(F32)
    part_b = rest.astype(BF16)
    part_c = (rest - part_b.astype(F32)).astype(BF16)
    wt_ref[0:router, :] = lax.dot_general(eye, wr, NT, preferred_element_type=F32).astype(BF16)
    tail = jnp.concatenate([part_a.astype(F32), part_b.astype(F32), part_c.astype(F32), jnp.zeros_like(folded)], axis=0)
    wt_ref[router:, :] = tail.astype(BF16)


def over_lanes(rows):
    cols = [jnp.transpose(jnp.broadcast_to(rows[r : r + 1], (LANES, LANES))) for r in range(rows.shape[0])]
    return jnp.concatenate(cols, axis=0)


def dispatch_kernel(
    router, num_experts, capacity, slots, tau_ref, ids_ref, ord_ref, wr_ref, keys_ref, x_ref,
    start_ref, count_ref, offset_ref, list_ref, pos_ref, gate_ref, xs_ref, wt_ref,
):
    grans = slots // GRAN
    spare = start_ref.shape[0] * grans

    @pl.when(pl.program_id(0) == 0)
    def _():
        plan_step(
            num_experts, capacity, grans, ids_ref, ord_ref, wr_ref, keys_ref,
            pos_ref, start_ref, count_ref, offset_ref, list_ref, wt_ref,
        )
        xs_ref[spare:] = jnp.zeros((xs_ref.shape[0] - spare,) + xs_ref.shape[1:], BF16)

    rows = x_ref.shape[0] // LANES
    part = pl.ds(pl.multiple_of(pl.program_id(0) * rows, rows), rows)
    ids, pos = ids_ref[part, :], pos_ref[part, :]
    tau = tau_ref[0, 0]
    for sub in range(rows // BLOCK_ROWS):
        row0 = sub * BLOCK_ROWS
        x = x_ref[row0 * LANES : (row0 + BLOCK_ROWS) * LANES, :]
        proj = lax.dot_general(wt_ref[...], x, NT, preferred_element_type=F32)
        square = jnp.sum(proj[:router] * proj[:router], axis=0, keepdims=True)
        ne = num_experts
        logits = proj[router : router + ne] + proj[router + ne : router + 2 * ne] + proj[router + 2 * ne : router + 3 * ne]
        logits = logits / jnp.sqrt(square) / tau
        expo = jnp.exp(logits - jnp.max(logits, axis=0, keepdims=True))
        prob = expo / jnp.sum(expo, axis=0, keepdims=True)
        id_row = jnp.concatenate([ids[r : r + 1] for r in range(row0, row0 + BLOCK_ROWS)], axis=1)
        gate = jnp.sum(jnp.where(iota(prob.shape, 0) == id_row, prob, 0.0), axis=0, keepdims=True)
        for r in range(BLOCK_ROWS):
            gate_ref[row0 + r : row0 + r + 1, :] = gate[:, r * LANES : (r + 1) * LANES]
        slot_iota = iota((slots, LANES), 0)
        hot = [(slot_iota == pos[r : r + 1]).astype(F32).astype(BF16) for r in range(row0, row0 + BLOCK_ROWS)]
        picked = jnp.dot(jnp.concatenate(hot, axis=1), x, preferred_element_type=F32).astype(BF16)
        at = pl.ds((pl.program_id(0) * (rows // BLOCK_ROWS) + sub) * grans, grans)
        xs_ref[at] = picked.reshape(grans, GRAN, picked.shape[1])


def expert_names(bits):
    me = lax.axis_index("ep_b") * lax.axis_size("ep_a") + lax.axis_index("ep_a")
    return [me ^ bit for bit in bits]


def stacked_dot(left, refs, columns):
    total, at = None, 0
    for ref in refs:
        depth = min(ref.shape[0], left.shape[1] - at)
        part = jnp.dot(left[:, at : at + depth], ref[0:depth, columns], preferred_element_type=F32)
        total = part if total is None else total + part
        at += depth
    return total


def pack_kernel(w_ref, b1_ref, b2_ref, out_ref, b1_buf, b2_buf, sems):
    depth, hidden = w_ref.shape
    copies = [
        pltpu.make_async_copy(b1_ref, b1_buf, sems.at[0]),
        pltpu.make_async_copy(b2_ref, b2_buf, sems.at[1]),
        pltpu.make_async_copy(w_ref, out_ref.at[pl.ds(0, depth)], sems.at[2]),
    ]
    for copy in copies:
        copy.start()
    for copy in copies[:2]:
        copy.wait()
    b2 = b2_buf[...].astype(F32)
    b2 = jnp.concatenate([b2, jnp.zeros((1, hidden - b2.shape[1]), F32)], axis=1)
    row = iota((EXTRA, hidden), 0)
    lines = jnp.where(row == 0, b1_buf[...].astype(F32), jnp.where(row == 1, b2, 0.0))
    out_ref[depth:, :] = lines.astype(BF16)
    copies[2].wait()


def split_bias(ref, width):
    lines = ref[ref.shape[0] - EXTRA :, :].astype(F32)
    return lines[0:1], lines[1:2, 0:width]


def up_tile(x, refs, b1, h_ref, at):
    hidden = refs[0].shape[1]
    step = 256
    for c in range(0, hidden, step):
        pre = stacked_dot(x, refs, slice(c, c + step)) + b1[:, c : c + step]
        act = 0.5 * pre * (1.0 + lax.erf(pre * F32(0.5**0.5)))
        h_ref[at, c : c + step] = act.astype(BF16)


def granules(e, count_ref, offset_ref):
    last = count_ref.shape[0] - 1
    return offset_ref[last, e] + count_ref[last, e]


def tile_names(e, start, tile, list_ref):
    return [list_ref[e, start + k] for k in range(tile)]


def tile_start(t, tile, most):
    return jnp.minimum(t * tile, most - tile)


def tile_rows(i, start, tile, most):
    return pl.ds(pl.multiple_of((i * most + start) * GRAN, GRAN), tile * GRAN)


def put_rows(names, spare, y, out_ref):
    for k, name in enumerate(names):
        out_ref[jnp.where(name == spare, spare + 15, name)] = y[k * GRAN : (k + 1) * GRAN]


def expert_kernel(bits, tile, spare, count_ref, offset_ref, list_ref, xs_ref, *refs):
    count = len(bits)
    w1_refs, w2_refs = refs[:count], refs[count : 2 * count]
    out_ref, h_buf = refs[2 * count :]
    for i, e in enumerate(expert_names(bits)):
        b1, b2 = split_bias(w1_refs[i], xs_ref.shape[2])

        def per_tile(t, _):
            names = tile_names(e, t * tile, tile, list_ref)
            up_tile(jnp.concatenate([xs_ref[name] for name in names], axis=0), [w1_refs[i]], b1, h_buf, slice(None))
            y = stacked_dot(h_buf[...], [w2_refs[i]], slice(None)) + b2
            put_rows(names, spare, y.astype(BF16), out_ref)
            return 0

        lax.fori_loop(0, (granules(e, count_ref, offset_ref) + tile - 1) // tile, per_tile, 0)


def up_kernel(bits, pieces, tile, most, count_ref, offset_ref, list_ref, xs_ref, *refs):
    count = len(bits)
    w1_refs = [refs[i * pieces : (i + 1) * pieces] for i in range(count)]
    h_ref, b2_ref = refs[count * pieces :]
    width = b2_ref.shape[1]
    for i, e in enumerate(expert_names(bits)):
        b1, b2 = split_bias(w1_refs[i][-1], width)
        b2_ref[i * EXTRA : (i + 1) * EXTRA, :] = jnp.broadcast_to(b2, (EXTRA, width))

        def per_tile(t, _):
            start = tile_start(t, tile, most)
            names = tile_names(e, start, tile, list_ref)
            at = tile_rows(i, start, tile, most)
            up_tile(jnp.concatenate([xs_ref[name] for name in names], axis=0), w1_refs[i], b1, h_ref, at)
            return 0

        lax.fori_loop(0, (granules(e, count_ref, offset_ref) + tile - 1) // tile, per_tile, 0)


def down_kernel(bits, first, tile, most, spare, count_ref, offset_ref, list_ref, xs_ref, h_ref, *refs):
    count = len(bits)
    b2_ref, w2_refs, out_ref = refs[0], refs[1 : count + 1], refs[count + 1]
    del xs_ref
    for i, e in enumerate(expert_names(bits)):
        b2 = b2_ref[(first + i) * EXTRA : (first + i) * EXTRA + 1, :]

        def per_tile(t, _):
            start = tile_start(t, tile, most)
            names = tile_names(e, start, tile, list_ref)
            at = tile_rows(first + i, start, tile, most)
            y = stacked_dot(h_ref[at, :], [w2_refs[i]], slice(None)) + b2
            put_rows(names, spare, y.astype(BF16), out_ref)
            return 0

        lax.fori_loop(0, (granules(e, count_ref, offset_ref) + tile - 1) // tile, per_tile, 0)


def compact_down(total, tile, most, window, w2_refs, b2_ref, h_ref, y_ref, after=lambda t, state: state):
    width = y_ref.shape[2]
    b2 = b2_ref[0:1, :]

    def per_tile(t, state):
        start = tile_start(t, tile, most)
        y = stacked_dot(h_ref[tile_rows(0, start, tile, most), :], w2_refs, slice(None)) + b2
        y_ref[pl.ds(start, tile)] = y.astype(BF16).reshape(tile, GRAN, width)
        y_ref[pl.ds(start + tile, window)] = jnp.zeros((window, GRAN, width), BF16)
        return after(t, state)

    tiles = (total + tile - 1) // tile

    @pl.when(tiles == 0)
    def _():
        y_ref[pl.ds(0, window)] = jnp.zeros((window, GRAN, width), BF16)

    return lax.fori_loop(0, tiles, per_tile, jnp.int32(0))


def half_kernel(bits, tile, most, window, count_ref, offset_ref, h_ref, *refs):
    total = granules(expert_names(bits)[0], count_ref, offset_ref)
    compact_down(total, tile, most, window, refs[:-2], refs[-2], h_ref, refs[-1])


def final_kernel(bits, tile, most, window, start_ref, count_ref, offset_ref, slot_ref, gate_ref, h_ref, part_ref, y_ref, *refs):
    experts = expert_names(bits)
    out_ref, y_buf, o_buf, o_sem = refs[-4:]
    y_refs = (y_ref, y_buf)
    blocks = start_ref.shape[0]
    width = part_ref.shape[1]
    block_tok = BLOCK_ROWS * LANES
    totals = [granules(e, count_ref, offset_ref) for e in experts]

    def rows_of(i, w, b):
        at = jnp.minimum(offset_ref[b, experts[i]] + w * window, totals[i])
        return y_refs[i][pl.ds(at, window)].reshape(window * GRAN, width)

    def out_copy(b, turn, sub):
        rows = pl.ds(pl.multiple_of(b * block_tok, block_tok), block_tok)
        part = o_buf.at[turn, pl.ds(sub * block_tok, block_tok)]
        return pltpu.make_async_copy(part, out_ref.at[rows], o_sem.at[turn, sub])

    def add(b, w, sub, turn, slots, gates, base_ref, base_at):
        part = slice(sub * BLOCK_ROWS, (sub + 1) * BLOCK_ROWS)
        back = window_dot(experts, w, b, start_ref, count_ref, over_lanes(slots[part]), rows_of)
        gate = over_lanes(gates[part])
        for c in range(0, width, LANES):
            scaled = (back[:, c : c + LANES] * gate).astype(BF16)
            o_buf[turn, sub * block_tok : (sub + 1) * block_tok, c : c + LANES] = base_ref[base_at, c : c + LANES] + scaled

    def per_pair(pair, _):
        turn = pair % 2
        rows8 = pl.ds(pl.multiple_of(pair * 2 * BLOCK_ROWS, 2 * BLOCK_ROWS), 2 * BLOCK_ROWS)
        slots, gates = slot_ref[rows8, :].astype(F32), gate_ref[rows8, :]

        @pl.when(pair >= 2)
        def _():
            for sub in range(2):
                out_copy(2 * pair + sub, turn, sub).wait()

        for sub in range(2):
            b = 2 * pair + sub
            add(b, 0, sub, turn, slots, gates, part_ref, pl.ds(pl.multiple_of(b * block_tok, block_tok), block_tok))
        for sub in range(2):
            b = 2 * pair + sub

            def more(w, _):
                add(b, w, sub, turn, slots, gates, o_buf.at[turn], slice(sub * block_tok, (sub + 1) * block_tok))
                return 0

            lax.fori_loop(1, (longest_run(experts, b, count_ref) + window - 1) // window, more, 0)
            out_copy(b, turn, sub).start()
        return 0

    def ready_pairs(t, done):
        ready = 0
        for pair in range(blocks // 2):
            end = offset_ref[2 * pair + 1, experts[-1]] + count_ref[2 * pair + 1, experts[-1]]
            ready = ready + jnp.where(end <= (t + 1) * tile, 1, 0)
        lax.fori_loop(done, ready, per_pair, 0)
        return ready

    done = compact_down(totals[-1], tile, most, window, refs[:-5], refs[-5], h_ref, y_buf, ready_pairs)
    lax.fori_loop(done, blocks // 2, per_pair, 0)
    for turn in range(2):
        for sub in range(2):
            out_copy(0, turn, sub).wait()


def window_dot(experts, w, b, start_ref, count_ref, slot, rows_of):
    lane = iota((1, LANES), 1)
    hot = []
    for e in experts:
        index = lane + w * LANES
        name = jnp.where(index < count_ref[b, e] * GRAN, index + start_ref[b, e] * GRAN, -2)
        hot.append((slot == name.astype(F32)).astype(F32).astype(BF16))
    return jnp.dot(jnp.concatenate(hot, axis=1), jnp.concatenate([rows_of(e, w, b) for e in range(len(experts))], axis=0), preferred_element_type=F32)


def longest_run(experts, b, count_ref):
    longest = count_ref[b, experts[0]]
    for e in experts[1:]:
        longest = jnp.maximum(longest, count_ref[b, e])
    return longest


def part_kernel(bits, fresh, window, span, start_ref, count_ref, xs_ref, slot_ref, gate_ref, *refs):
    experts = expert_names(bits)
    out_ref = refs[-1]
    width = xs_ref.shape[2]
    block_tok = BLOCK_ROWS * LANES

    def rows_of(i, w, b):
        at = jnp.minimum(b * span + start_ref[b, experts[i]] + w * window, xs_ref.shape[0] - 1 - window)
        return xs_ref[pl.ds(at, window)].reshape(window * GRAN, width)

    def add(b, w, slot, gate, fresh):
        back = window_dot(experts, w, b, start_ref, count_ref, slot, rows_of)
        at = pl.ds(pl.multiple_of(b * block_tok, block_tok), block_tok)
        for c in range(0, width, LANES):
            scaled = (back[:, c : c + LANES] * gate).astype(BF16)
            if not fresh:
                scaled = scaled + out_ref[at, c : c + LANES]
            out_ref[at, c : c + LANES] = scaled

    def per_group(group, _):
        row0 = pl.multiple_of(group * 4 * BLOCK_ROWS, 4 * BLOCK_ROWS)
        slots = slot_ref[pl.ds(row0, 4 * BLOCK_ROWS), :].astype(F32)
        gates = gate_ref[pl.ds(row0, 4 * BLOCK_ROWS), :]
        for sub in range(4):
            part = slice(sub * BLOCK_ROWS, (sub + 1) * BLOCK_ROWS)
            add(4 * group + sub, 0, over_lanes(slots[part]), over_lanes(gates[part]), fresh)
        for sub in range(4):
            part = slice(sub * BLOCK_ROWS, (sub + 1) * BLOCK_ROWS)

            def more(w, _):
                add(4 * group + sub, w, over_lanes(slots[part]), over_lanes(gates[part]), False)
                return 0

            lax.fori_loop(1, (longest_run(experts, 4 * group + sub, count_ref) + window - 1) // window, more, 0)
        return 0

    lax.fori_loop(0, start_ref.shape[0] // 4, per_group, 0)


def vmem():
    return pl.BlockSpec(memory_space=pltpu.VMEM)


def smem():
    return pl.BlockSpec(memory_space=pltpu.SMEM)


def hbm():
    return pl.BlockSpec(memory_space=pl.ANY)


def solution(mesh):
    num_experts = mesh.shape["ep_b"] * mesh.shape["ep_a"]
    tok_spec = P(("dp",) + EXPERT_AXES)
    expert_spec = P(EXPERT_AXES)

    def swap(value, bit):
        return lax.ppermute(value, EXPERT_AXES, [(e, e ^ bit) for e in range(num_experts)])

    def inner_step(tokens, expert_ids, route_order, w_route, expert_keys, value_a11, w_in, b_in, w_out, b_out):
        tok_dev, width = tokens.shape[1], tokens.shape[2]
        hidden = w_in.shape[2]
        router = w_route.shape[1]
        capacity = (5 * tok_dev + 4 * num_experts - 1) // (4 * num_experts)
        rows = tok_dev // LANES
        blocks = rows // BLOCK_ROWS
        slots = -(-(BLOCK_ROWS * LANES + num_experts * (GRAN - 1)) // LANES) * LANES
        span = slots // GRAN

        second = w_out[0]
        first = pl.pallas_call(
            pack_kernel,
            out_shape=pltpu.VMEM((width + EXTRA, hidden), BF16),
            in_specs=[hbm()] * 3,
            out_specs=vmem(),
            scratch_shapes=[pltpu.VMEM((1, hidden), BF16), pltpu.VMEM((1, width), BF16), pltpu.SemaphoreType.DMA((3,))],
            compiler_params=pltpu.CompilerParams(vmem_limit_bytes=LIMIT * 2**20),
            name="pack",
        )(*[pltpu.with_memory_space_constraint(array, pltpu.HBM) for array in (w_in[0], b_in, b_out)])
        x_first, y_first = swap(first, 2), swap(first, 4)
        x_second, y_second = swap(second, 2), swap(second, 4)
        c_first, c_second = swap(first, 1), swap(second, 1)

        ids, order = expert_ids.reshape(rows, LANES), route_order.reshape(rows, LANES)
        unit = 2 * BLOCK_ROWS
        small = functools.partial(pl.BlockSpec, index_map=lambda i: (0, 0))
        whole = small((rows, LANES))
        table = small((blocks, LANES))
        xs_shape = (blocks * span + 16, GRAN, width)
        starts, counts, offsets, lists, slot, gate, xs = pl.pallas_call(
            functools.partial(dispatch_kernel, router, num_experts, capacity, slots),
            out_shape=(
                jax.ShapeDtypeStruct((blocks, LANES), jnp.int32),
                jax.ShapeDtypeStruct((blocks, LANES), jnp.int32),
                jax.ShapeDtypeStruct((blocks, LANES), jnp.int32),
                jax.ShapeDtypeStruct((num_experts, LANES), jnp.int32),
                jax.ShapeDtypeStruct((rows, LANES), jnp.int32),
                jax.ShapeDtypeStruct((rows, LANES), F32),
                pltpu.VMEM(xs_shape, BF16),
            ),
            grid=(rows // unit,),
            in_specs=[
                smem(),
                whole,
                whole,
                small((width, router)),
                small((num_experts, router)),
                pl.BlockSpec((unit * LANES, width), lambda i: (i, 0)),
            ],
            out_specs=(
                table, table, table, small((num_experts, LANES)),
                whole, pl.BlockSpec((unit, LANES), lambda i: (i, 0)), vmem(),
            ),
            scratch_shapes=[pltpu.VMEM((router + 4 * num_experts, width), BF16)],
            cost_estimate=pl.CostEstimate(flops=9 * 10**9, bytes_accessed=14 * 10**6, transcendentals=0),
            compiler_params=pltpu.CompilerParams(vmem_limit_bytes=12 * 2**20),
            name="dispatch",
        )(value_a11.reshape(1, 1), *[pltpu.with_memory_space_constraint(array, pltpu.HBM) for array in (ids, order, w_route, expert_keys, tokens[0])])

        most = -(-(capacity + blocks * (GRAN - 1)) // (16 * GRAN)) * 16
        tile, window = TILE, 8
        held = lambda array: pltpu.with_memory_space_constraint(array, pltpu.VMEM)

        spare = blocks * span
        limit = pltpu.CompilerParams(vmem_limit_bytes=LIMIT * 2**20)
        tables = (counts, offsets, lists)

        def cost(flops):
            return pl.CostEstimate(flops=flops, bytes_accessed=10**6, transcendentals=0)

        def up(bits, xs, firsts):
            n = len(bits)
            pieces = len(firsts[0])
            return pl.pallas_call(
                functools.partial(up_kernel, bits, pieces, tile, most),
                out_shape=(pltpu.VMEM((n * most * GRAN, hidden), BF16), jax.ShapeDtypeStruct((n * EXTRA, width), F32)),
                in_specs=[smem()] * 3 + [vmem()] * (1 + n * pieces),
                out_specs=(vmem(), vmem()),
                cost_estimate=cost(2 * n * 10**9),
                compiler_params=limit,
            )(*tables, held(xs), *[held(piece) for expert in firsts for piece in expert])

        def down(bits, place, xs, h, b2, seconds):
            return pl.pallas_call(
                functools.partial(down_kernel, bits, place, tile, most, spare),
                out_shape=pltpu.VMEM(xs.shape, BF16),
                in_specs=[smem()] * 3 + [vmem()] * (3 + len(bits)),
                out_specs=vmem(),
                input_output_aliases={3: 0},
                cost_estimate=cost(2 * len(bits) * 10**9),
                compiler_params=limit,
            )(*tables, held(xs), held(h), b2, *map(held, seconds))

        def partial(bits, xs, part):
            held_part = [] if part is None else [held(part)]
            return pl.pallas_call(
                functools.partial(part_kernel, bits, part is None, window, span),
                out_shape=pltpu.VMEM((tok_dev, width), BF16),
                in_specs=[smem()] * 2 + [vmem()] * (3 + len(held_part)),
                out_specs=vmem(),
                input_output_aliases={} if part is None else {5: 0},
                cost_estimate=cost(2 * len(bits) * 10**9),
                compiler_params=limit,
            )(starts, counts, held(xs), slot, gate, *held_part)

        xs = pl.pallas_call(
            functools.partial(expert_kernel, (0, 1), tile, spare),
            out_shape=pltpu.VMEM(xs.shape, BF16),
            in_specs=[smem()] * 3 + [vmem()] * 5,
            out_specs=vmem(),
            scratch_shapes=[pltpu.VMEM((tile * GRAN, hidden), BF16)],
            input_output_aliases={3: 0},
            cost_estimate=cost(6 * 10**9),
            compiler_params=pltpu.CompilerParams(vmem_limit_bytes=2 * LIMIT * 2**20),
            name="experts0",
        )(*tables, held(xs), held(first), held(c_first), held(second), held(c_second))
        x_first, y_first, xs = lax.optimization_barrier((x_first, y_first, xs))
        cut = width - LANES
        d_top, d_low = swap(x_first[:cut], 4), swap(y_first[cut:], 2)
        cx_first, cy_first = swap(x_first, 1), swap(y_first, 1)
        h, b2 = up((2, 4, 3, 5), xs, ((x_first,), (y_first,), (cx_first,), (cy_first,)))
        part = partial((0, 1), xs, None)
        x_second, y_second, h, part = lax.optimization_barrier((x_second, y_second, h, part))
        edge = hidden // 3
        e_top, e_low = swap(x_second[:edge], 4), swap(y_second[edge:], 2)
        cx_second, cy_second = swap(x_second, 1), swap(y_second, 1)
        xs = down((2, 4), 0, xs, h, b2, (x_second, y_second))
        xs = down((3, 5), 2, xs, h, b2, (cx_second, cy_second))
        part = partial((2, 4, 3, 5), xs, part)
        d_top, d_low, part = lax.optimization_barrier((d_top, d_low, part))
        cd_top, cd_low = swap(d_top, 1), swap(d_low, 1)
        h6, b6 = up((6,), xs, ((d_top, d_low),))
        h6, cd_top, cd_low = lax.optimization_barrier((h6, cd_top, cd_low))
        h7, b7 = up((7,), xs, ((cd_top, cd_low),))
        e_top, e_low, h6, h7 = lax.optimization_barrier((e_top, e_low, h6, h7))
        ce_top, ce_low = swap(e_top, 1), swap(e_low, 1)
        y = pl.pallas_call(
            functools.partial(half_kernel, (6,), tile, most, window),
            out_shape=pltpu.VMEM((most + window, GRAN, width), BF16),
            in_specs=[smem()] * 2 + [vmem()] * 4,
            out_specs=vmem(),
            cost_estimate=cost(2 * 10**9),
            compiler_params=limit,
            name="half",
        )(counts, offsets, held(h6), held(e_top), held(e_low), b6)
        out = pl.pallas_call(
            functools.partial(final_kernel, (6, 7), tile, most, window),
            out_shape=jax.ShapeDtypeStruct((tok_dev, width), BF16),
            in_specs=[smem()] * 3 + [vmem()] * (5 + 3),
            out_specs=hbm(),
            scratch_shapes=[
                pltpu.VMEM((most + window, GRAN, width), BF16),
                pltpu.VMEM((2, 2 * BLOCK_ROWS * LANES, width), BF16),
                pltpu.SemaphoreType.DMA((2, 2)),
            ],
            cost_estimate=cost(5 * 10**9),
            compiler_params=pltpu.CompilerParams(vmem_limit_bytes=7 * 2**20),
            name="final",
        )(starts, counts, offsets, slot, gate, held(h7), held(part), held(y), held(ce_top), held(ce_low), b7)
        return out[None]

    return jax.shard_map(
        inner_step,
        mesh=mesh,
        in_specs=(tok_spec, tok_spec, tok_spec, P(), P(), P(), expert_spec, expert_spec, expert_spec, expert_spec),
        out_specs=tok_spec,
        check_vma=False,
    )
```
